16 devices in a mesh: dp: 4 (over z, y), tp: 4 (over x, core).
Axes of the slice: x: 2, y: 2, z: 2, core: 2. Of those that a mesh axis runs over, the one named last changes fastest.
Arguments:
- hidden: bfloat16 [64, 5, 5120], P('dp'), parts along dimension 0
- draft_ids: int32 [64, 4], P('dp'), parts along dimension 0
- norm_gain: bfloat16 [5120], replicated
- head_w: bfloat16 [5120, 32000], P(None, 'tp')
Outputs:
- output 1: float32 [64, 4], P('dp'), parts along dimension 0
- output 2: float32 [64, 5], P('dp'), parts along dimension 0
- output 3: float32 [64, 5], P('dp'), parts along dimension 0
There are 4 independent parts. The reference program is written for one: setup_inputs(seed, part) draws one part's arguments, and reference() takes and returns one part's arrays. A program takes and returns all parts, laid end to end along the dimension named above; an argument that names none is the same for every part.
All inputs are finite; a program needn't handle non-finite values.
Results may differ from the reference program's by a relative error of at most 0.001.
Values sent between devices are 32-bit elements.
A program may use at most 1 GiB of HBM per device.

```python
import jax
import jax.numpy as jnp
from jax import lax

DIM = 5120
VOCAB = 32000
BATCH = 16
DRAFTS = 4
NORM_EPS = 1e-5


def setup_inputs(seed: int = 0, part: int = 0) -> dict:
    root_key = jax.random.key(seed)
    shared_key, part_base = jax.random.split(root_key)
    part_key = jax.random.fold_in(part_base, part)
    key_x, key_d = jax.random.split(part_key)
    key_g, key_w, key_hot = jax.random.split(shared_key, 3)
    hidden = jax.random.normal(key_x, (BATCH, DRAFTS + 1, DIM), jnp.float32)
    draft_ids = jax.random.randint(key_d, (BATCH, DRAFTS), 0, VOCAB, jnp.int32)
    norm_gain = 1.0 + 0.2 * jax.random.normal(key_g, (DIM,), jnp.float32)
    hot_cols = jax.random.randint(key_hot, (VOCAB,), 0, 64, jnp.int32) == 0
    col_scale = jnp.where(hot_cols, 3.5, 2.0) * DIM ** -0.5
    head_w = jax.random.normal(key_w, (DIM, VOCAB), jnp.float32) * col_scale
    return {'hidden': hidden.astype(jnp.bfloat16), 'draft_ids': draft_ids, 'norm_gain': norm_gain.astype(jnp.bfloat16), 'head_w': head_w.astype(jnp.bfloat16)}


def rms_norm(hidden, norm_gain):
    wide_x = hidden.astype(jnp.float32)
    inv_rms = lax.rsqrt(jnp.mean(wide_x * wide_x, axis=-1, keepdims=True) + NORM_EPS)
    return (wide_x * inv_rms * norm_gain.astype(jnp.float32)).astype(jnp.bfloat16)


def reference(hidden, draft_ids, norm_gain, head_w):
    def one_sequence(seq_pair):
        seq_rows, seq_ids = seq_pair
        normed = rms_norm(seq_rows, norm_gain)
        logits = jnp.dot(normed, head_w, preferred_element_type=jnp.float32)
        row_max = jnp.max(logits, axis=-1)
        shifted = logits - row_max[:, None]
        exp_vals = jnp.exp(shifted)
        exp_sum = jnp.sum(exp_vals, axis=-1)
        weighted = jnp.sum(exp_vals * shifted, axis=-1)
        log_sum = jnp.log(exp_sum)
        log_norm = row_max + log_sum
        entropy = log_sum - weighted / exp_sum
        drafts = seq_ids.shape[0]
        picked = jnp.take_along_axis(logits[:drafts], seq_ids[:, None], axis=1)[:, 0]
        return picked - log_norm[:drafts], log_norm, entropy
    draft_logp, log_norm, entropy = lax.map(one_sequence, (hidden, draft_ids))
    return draft_logp, log_norm, entropy
```

```python
import jax
import jax.numpy as jnp
from jax import lax
from jax.experimental import pallas as pl
from jax.experimental.pallas import tpu as pltpu
from jax.sharding import PartitionSpec as P

NORM_EPS = 1e-5
MESH = pl.DeviceIdType.MESH
LANES = 128
SLOTS = 8
CHUNK = 400


def rows_sum(block):
    return jnp.sum(block.reshape(-1, 8, block.shape[-1]), axis=0)


def rows_max(block):
    return jnp.max(block.reshape(-1, 8, block.shape[-1]), axis=0)


def update_stats(first, z, row_ids, ids, carry):
    m, s, w, p = carry
    bm = rows_max(z)
    m = jnp.where(first, bm, m)
    mn = jnp.maximum(m, bm)
    dm = m - mn
    a = jnp.exp(dm)
    z3 = z.reshape(-1, 8, z.shape[-1])
    sh = z3 - mn[None]
    e = jnp.exp(sh)
    w = a * (w + dm * s) + jnp.sum(e * sh, axis=0)
    s = a * s + jnp.sum(e, axis=0)
    p = p + rows_sum(jnp.where(row_ids == ids, z, 0.0))
    return mn, s, w, p


def pack_stats(carry):
    m, s, w, p = carry
    top = jnp.max(m, axis=0, keepdims=True)
    dm = m - top
    f = jnp.exp(dm)
    return (
        top,
        jnp.sum(f * s, axis=0, keepdims=True),
        jnp.sum(f * (w + dm * s), axis=0, keepdims=True),
        jnp.sum(p, axis=0, keepdims=True),
    )


def solution(mesh):
    tp = mesh.shape['tp']

    def per_device(hidden, draft_ids, norm_gain, head_w):
        batch, pos, dim = hidden.shape
        drafts = draft_ids.shape[1]
        cols = head_w.shape[1]
        rows = batch * pos
        kblocks = dim // LANES
        chunks = cols // CHUNK

        def kernel(x_hbm, ids_hbm, g_hbm, w_hbm, o_logp, o_logn, o_ent,
                   wv, xv, nb, gv, gf, idv, sq, st, rs, wsem, lsem, ssem, rsem):
            t = lax.axis_index('tp')
            d = lax.axis_index('dp')
            cx = pltpu.make_async_copy(x_hbm, xv, lsem.at[0])
            cg = pltpu.make_async_copy(g_hbm, gv, lsem.at[1])
            ci = pltpu.make_async_copy(ids_hbm, idv, lsem.at[2])
            cx.start()
            cg.start()
            ci.start()

            def w_copy(j, slot):
                return pltpu.make_async_copy(
                    w_hbm.at[pl.ds(pl.multiple_of(j * CHUNK, CHUNK), CHUNK), :], wv.at[slot], wsem.at[slot])

            for j in range(SLOTS):
                w_copy(j, j).start()
            barrier = pltpu.get_barrier_semaphore()
            for k in range(1, tp):
                pl.semaphore_signal(barrier, inc=1, device_id=(d, lax.rem(t + k, tp)), device_id_type=MESH)
            nb[rows:, :] = jnp.zeros((LANES - rows, dim), jnp.bfloat16)
            cg.wait()
            gf[...] = gv[...].astype(jnp.float32)
            ci.wait()
            ids = jnp.concatenate([idv[k:k + 1, :] for k in range(drafts)]
                                  + [jnp.full((1, LANES - drafts * batch), -1, jnp.int32)], axis=1)
            ids = ids - t * cols
            cx.wait()
            acc = jnp.zeros((rows, LANES), jnp.float32)
            for k in range(kblocks):
                x = xv[:, k * LANES:(k + 1) * LANES].astype(jnp.float32)
                acc = acc + x * x
            inv = lax.rsqrt(jnp.sum(acc, axis=1, keepdims=True) / dim + NORM_EPS)
            for k in range(kblocks):
                x = xv[:, k * LANES:(k + 1) * LANES].astype(jnp.float32)
                nb[:rows, k * LANES:(k + 1) * LANES] = (x * inv * gf[k:k + 1, :]).astype(jnp.bfloat16)

            row_iota = lax.broadcasted_iota(jnp.int32, (CHUNK, LANES), 0)

            def step(j, carry):
                slot = lax.rem(j, SLOTS)
                w_copy(j, slot).wait()
                z = lax.dot_general(wv[slot], nb[...], (((1,), (1,)), ((), ())), preferred_element_type=jnp.float32)

                @pl.when(j + SLOTS < chunks)
                def _():
                    w_copy(j + SLOTS, slot).start()

                return update_stats(j == 0, z, row_iota, ids - j * CHUNK, carry)

            zero = jnp.zeros((8, LANES), jnp.float32)
            carry = lax.fori_loop(0, chunks, step, (zero, zero, zero, zero))
            packed = pack_stats(carry)
            for k in range(4):
                st[k:k + 1, :] = packed[k]
                rs[t, k:k + 1, :] = packed[k]
            pl.semaphore_wait(barrier, tp - 1)
            sends = []
            for k in range(1, tp):
                peer = lax.rem(t + k, tp)
                c = pltpu.make_async_remote_copy(
                    src_ref=st, dst_ref=rs.at[t], send_sem=ssem.at[k], recv_sem=rsem.at[t],
                    device_id=(d, peer), device_id_type=MESH)
                c.start()
                sends.append(c)
            for k in range(1, tp):
                peer = lax.rem(t + k, tp)
                pltpu.make_async_remote_copy(
                    src_ref=st, dst_ref=rs.at[peer], send_sem=ssem.at[k], recv_sem=rsem.at[peer],
                    device_id=(d, peer), device_id_type=MESH).wait_recv()
            ms = [rs[k, 0:1, :] for k in range(tp)]
            top = ms[0]
            for k in range(1, tp):
                top = jnp.maximum(top, ms[k])
            s = jnp.zeros((1, LANES), jnp.float32)
            w = s
            p = s
            for k in range(tp):
                dm = ms[k] - top
                f = jnp.exp(dm)
                s = s + f * rs[k, 1:2, :]
                w = w + f * (rs[k, 2:3, :] + dm * rs[k, 1:2, :])
                p = p + rs[k, 3:4, :]
            log_sum = jnp.log(s)
            log_norm = top + log_sum
            ent = log_sum - w / s
            logp = p - log_norm
            for k in range(pos):
                o_logn[k:k + 1, :] = log_norm[:, k * batch:(k + 1) * batch]
                o_ent[k:k + 1, :] = ent[:, k * batch:(k + 1) * batch]
            for k in range(drafts):
                o_logp[k:k + 1, :] = logp[:, k * batch:(k + 1) * batch]
            for c in sends:
                c.wait_send()

        hbm = pl.BlockSpec(memory_space=pl.ANY)
        vmem = pl.BlockSpec(memory_space=pltpu.VMEM)
        f32 = jnp.float32
        logp, logn, ent = pl.pallas_call(
            kernel,
            out_shape=[jax.ShapeDtypeStruct((drafts, batch), f32), jax.ShapeDtypeStruct((pos, batch), f32),
                       jax.ShapeDtypeStruct((pos, batch), f32)],
            in_specs=[hbm] * 4,
            out_specs=[vmem] * 3,
            scratch_shapes=[
                pltpu.VMEM((SLOTS, CHUNK, dim), jnp.bfloat16),
                pltpu.VMEM((rows, dim), jnp.bfloat16),
                pltpu.VMEM((LANES, dim), jnp.bfloat16),
                pltpu.VMEM((kblocks, LANES), jnp.bfloat16),
                pltpu.VMEM((kblocks, LANES), f32),
                pltpu.VMEM((drafts, batch), jnp.int32),
                pltpu.VMEM((8, LANES), f32),
                pltpu.VMEM((8, LANES), f32),
                pltpu.VMEM((tp, 8, LANES), f32),
                pltpu.SemaphoreType.DMA((SLOTS,)),
                pltpu.SemaphoreType.DMA((3,)),
                pltpu.SemaphoreType.DMA((tp,)),
                pltpu.SemaphoreType.DMA((tp,)),
            ],
            compiler_params=pltpu.CompilerParams(
                collective_id=0, has_side_effects=True, vmem_limit_bytes=60 * 1024 * 1024),
        )(hidden.transpose(1, 0, 2).reshape(rows, dim), draft_ids.T, norm_gain.reshape(kblocks, LANES), head_w.T)
        return logp.T, logn.T, ent.T

    specs_in = (P('dp', None, None), P('dp', None), P(None), P(None, 'tp'))
    specs_out = (P('dp', None), P('dp', None), P('dp', None))
    return jax.shard_map(per_device, mesh=mesh, in_specs=specs_in, out_specs=specs_out, check_vma=False)
```

```python
import jax
import jax.numpy as jnp
from jax import lax
from jax.experimental import pallas as pl
from jax.experimental.pallas import tpu as pltpu
from jax.sharding import PartitionSpec as P

NORM_EPS = 1e-5
MESH = pl.DeviceIdType.MESH
LANES = 128
TILE = 256
BLOCK = 800
NT = (((1,), (1,)), ((), ()))


def rows_sum(block):
    return jnp.sum(block.reshape(-1, 8, block.shape[-1]), axis=0)


def rows_max(block):
    return jnp.max(block.reshape(-1, 8, block.shape[-1]), axis=0)


def update_stats(z, row_ids, ids, carry):
    bm = rows_max(z)
    z3 = z.reshape(-1, 8, z.shape[-1])
    picked = rows_sum(jnp.where(row_ids == ids, z, 0.0))
    if carry is None:
        sh = z3 - bm[None]
        e = jnp.exp(sh)
        return bm, jnp.sum(e, axis=0), jnp.sum(e * sh, axis=0), picked
    m, s, w, p = carry
    mn = jnp.maximum(m, bm)
    dm = m - mn
    a = jnp.exp(dm)
    sh = z3 - mn[None]
    e = jnp.exp(sh)
    w = a * (w + dm * s) + jnp.sum(e * sh, axis=0)
    s = a * s + jnp.sum(e, axis=0)
    return mn, s, w, p + picked


def pack_stats(carry):
    m, s, w, p = carry
    top = jnp.max(m, axis=0, keepdims=True)
    dm = m - top
    f = jnp.exp(dm)
    return (
        top,
        jnp.sum(f * s, axis=0, keepdims=True),
        jnp.sum(f * (w + dm * s), axis=0, keepdims=True),
        jnp.sum(p, axis=0, keepdims=True),
    )


def solution(mesh):
    tp = mesh.shape['tp']

    def per_device(hidden, draft_ids, norm_gain, head_w):
        batch, pos, dim = hidden.shape
        drafts = draft_ids.shape[1]
        cols = head_w.shape[1]
        half = cols // 2
        rows = batch * pos
        kblocks = dim // LANES
        tiles = dim // TILE
        parts = kblocks // tp
        ptiles = tiles // tp
        nblocks = half // BLOCK
        f32 = jnp.float32

        def kernel(x_hbm, ids_hbm, g_hbm, w_hbm, o_logp, o_logn, o_ent,
                   wv, xv, nb, nf, pf, acc, gv, gf, idv, idp, st, rs,
                   wsem, lsem, ysend, yrecv, xsend, xrecv, asend, arecv, bsend, brecv, isend, irecv, ssem, rsem):
            t = lax.axis_index('tp')
            d = lax.axis_index('dp')
            y = lax.rem(d, 2)
            core = lax.rem(t, 2)
            mate = (d + 1 - 2 * y, t)
            sib = (d, t + 1 - 2 * core)
            nbr_t = lax.rem(t + 2, tp)
            nbr = (d, nbr_t)
            sib_t = t + 1 - 2 * core
            far_t = lax.rem(sib_t + 2, tp)

            cx = pltpu.make_async_copy(x_hbm, xv, lsem.at[0])
            cg = pltpu.make_async_copy(g_hbm, gv, lsem.at[1])
            ci = pltpu.make_async_copy(ids_hbm, idv, lsem.at[2])
            cx.start()
            cg.start()
            ci.start()

            def w_copy(kt):
                return pltpu.make_async_copy(
                    w_hbm.at[pl.ds(pl.multiple_of(y * half, 16), half), pl.ds(pl.multiple_of(kt * TILE, TILE), TILE)],
                    wv.at[kt], wsem.at[kt])

            def tile_of(stream_t, i):
                return stream_t * ptiles + i

            order = []
            for k in range(ptiles + 2):
                for s, i in ((t, k), (far_t, k - 2), (sib_t, k), (nbr_t, k - 1)):
                    if 0 <= i < ptiles:
                        order.append(tile_of(s, i))
            for kt in order:
                w_copy(kt).start()

            barrier = pltpu.get_barrier_semaphore()
            peers = []
            for dy in range(2):
                for k in range(tp):
                    if dy or k:
                        peers.append((mate[0] if dy else d, lax.rem(t + k, tp), dy, k))
            for pd, pt, _, _ in peers:
                pl.semaphore_signal(barrier, inc=1, device_id=(pd, pt), device_id_type=MESH)

            def y_copy(i):
                return pltpu.make_async_remote_copy(
                    src_ref=nf.at[i], dst_ref=pf.at[t * parts + i], send_sem=ysend.at[i], recv_sem=yrecv.at[i],
                    device_id=mate, device_id_type=MESH)

            def x_copy(i, owner):
                kb = owner * parts + i
                return pltpu.make_async_remote_copy(
                    src_ref=pf.at[kb], dst_ref=pf.at[kb], send_sem=xsend.at[i], recv_sem=xrecv.at[i],
                    device_id=nbr, device_id_type=MESH)

            def a_copy(i, owner):
                kb = owner * parts + i
                return pltpu.make_async_remote_copy(
                    src_ref=pf.at[kb], dst_ref=pf.at[kb], send_sem=asend.at[i], recv_sem=arecv.at[i],
                    device_id=sib, device_id_type=MESH)

            def b_copy(i, owner):
                kb = owner * parts + i
                return pltpu.make_async_remote_copy(
                    src_ref=pf.at[kb], dst_ref=pf.at[kb], send_sem=bsend.at[i], recv_sem=brecv.at[i],
                    device_id=sib, device_id_type=MESH)

            id_copy = pltpu.make_async_remote_copy(
                src_ref=idv, dst_ref=idp, send_sem=isend, recv_sem=irecv, device_id=mate, device_id_type=MESH)

            nb[rows:LANES, :] = jnp.zeros((LANES - rows, dim), jnp.bfloat16)
            nb[LANES + rows:, :] = jnp.zeros((LANES - rows, dim), jnp.bfloat16)
            cg.wait()
            gf[...] = gv[...].astype(f32)
            cx.wait()
            sq = jnp.zeros((rows, LANES), f32)
            for k in range(kblocks):
                x = xv[:, k * LANES:(k + 1) * LANES].astype(f32)
                sq = sq + x * x
            inv = lax.rsqrt(jnp.sum(sq, axis=1, keepdims=True) / dim + NORM_EPS)

            def normed(kb):
                x = xv[:, pl.ds(pl.multiple_of(kb * LANES, LANES), LANES)].astype(f32)
                return (x * inv * gf[pl.ds(kb, 1), :]).astype(jnp.bfloat16)

            for i in range(parts):
                nf[i] = normed(t * parts + i).astype(f32)
            ci.wait()
            pl.semaphore_wait(barrier, len(peers))
            for i in range(parts):
                y_copy(i).start()
            id_copy.start()
            for k in range(kblocks):
                nb[:rows, k * LANES:(k + 1) * LANES] = normed(k)
            acc[...] = jnp.zeros_like(acc)

            def forward_y(i):
                y_copy(i).wait_recv()
                x_copy(i, t).start()
                a_copy(i, t).start()

            def forward_x(i):
                x_copy(i, nbr_t).wait_recv()
                b_copy(i, nbr_t).start()

            def load_tile(kt):
                w_copy(kt).wait()
                for h in range(2):
                    nb[LANES:LANES + rows, pl.ds(pl.multiple_of(kt * TILE + h * LANES, LANES), LANES)] = (
                        pf[2 * kt + h].astype(jnp.bfloat16))

            def tile_dot(kt, r):
                return lax.dot_general(wv[kt, r, :], nb[:, pl.ds(pl.multiple_of(kt * TILE, TILE), TILE)], NT,
                                       preferred_element_type=f32)

            forward_y(0)

            def step(p, _):
                k = p // 2
                first = lax.rem(p, 2) == 0

                @pl.when(p + 1 < parts)
                def _():
                    forward_y(p + 1)

                @pl.when((p >= 2) & (p - 2 < parts))
                def _():
                    forward_x(p - 2)

                late = jnp.where(first, k - 2, k - 1)
                early_on = k < ptiles
                late_on = late >= 0
                early_t = tile_of(jnp.where(first, t, sib_t), k)
                late_t = tile_of(jnp.where(first, far_t, nbr_t), late)

                @pl.when((p % 2 == 1) & early_on)
                def _():
                    a_copy(2 * k, sib_t).wait_recv()
                    a_copy(2 * k + 1, sib_t).wait_recv()

                @pl.when((p % 2 == 0) & late_on)
                def _():
                    b_copy(2 * late, far_t).wait_recv()
                    b_copy(2 * late + 1, far_t).wait_recv()

                @pl.when(early_on & late_on)
                def _():
                    load_tile(early_t)
                    load_tile(late_t)
                    for n in range(nblocks):
                        r = slice(n * BLOCK, (n + 1) * BLOCK)
                        acc[r, :] = acc[r, :] + (tile_dot(early_t, r) + tile_dot(late_t, r))

                @pl.when(jnp.logical_not(early_on & late_on))
                def _():
                    one = jnp.where(early_on, early_t, late_t)
                    load_tile(one)
                    for n in range(nblocks):
                        r = slice(n * BLOCK, (n + 1) * BLOCK)
                        acc[r, :] = acc[r, :] + tile_dot(one, r)

                return 0

            lax.fori_loop(0, 2 * ptiles + 2, step, 0)

            pad = jnp.full((1, LANES - drafts * batch), -1, jnp.int32)
            id_copy.wait_recv()
            ids = jnp.concatenate([idv[k:k + 1, :] for k in range(drafts)] + [pad]
                                  + [idp[k:k + 1, :] for k in range(drafts)] + [pad], axis=1)
            ids = ids - (t * cols + y * half)
            row_iota = lax.broadcasted_iota(jnp.int32, (BLOCK, TILE), 0)
            last_t = tile_of(far_t, ptiles - 1)
            b_copy(parts - 2, far_t).wait_recv()
            b_copy(parts - 1, far_t).wait_recv()
            load_tile(last_t)
            carry = None
            for n in range(nblocks):
                r = slice(n * BLOCK, (n + 1) * BLOCK)
                z = acc[r, :] + tile_dot(last_t, r)
                carry = update_stats(z, row_iota, ids - n * BLOCK, carry)
            packed = pack_stats(carry)
            slot = y * tp + t
            for k in range(4):
                st[0, k:k + 1, :] = packed[k][:, :LANES]
                st[1, k:k + 1, :] = packed[k][:, LANES:]
                rs[slot, k:k + 1, :] = packed[k][:, :LANES]

            def s_copy(pd, pt, dy, k, into):
                return pltpu.make_async_remote_copy(
                    src_ref=st.at[dy], dst_ref=rs.at[into], send_sem=ssem.at[dy * tp + k], recv_sem=rsem.at[into],
                    device_id=(pd, pt), device_id_type=MESH)

            for pd, pt, dy, k in peers:
                s_copy(pd, pt, dy, k, slot).start()
            for i in range(parts):
                y_copy(i).wait_send()
                x_copy(i, t).wait_send()
                a_copy(i, t).wait_send()
                b_copy(i, nbr_t).wait_send()
            id_copy.wait_send()
            for pd, pt, dy, k in peers:
                s_copy(pd, pt, dy, k, (1 - y if dy else y) * tp + pt).wait_recv()
            ms = [rs[k, 0:1, :] for k in range(2 * tp)]
            top = ms[0]
            for k in range(1, 2 * tp):
                top = jnp.maximum(top, ms[k])
            s = jnp.zeros((1, LANES), f32)
            w = s
            p = s
            for k in range(2 * tp):
                dm = ms[k] - top
                f = jnp.exp(dm)
                s = s + f * rs[k, 1:2, :]
                w = w + f * (rs[k, 2:3, :] + dm * rs[k, 1:2, :])
                p = p + rs[k, 3:4, :]
            log_sum = jnp.log(s)
            log_norm = top + log_sum
            ent = log_sum - w / s
            logp = p - log_norm
            for k in range(pos):
                o_logn[k:k + 1, :] = log_norm[:, k * batch:(k + 1) * batch]
                o_ent[k:k + 1, :] = ent[:, k * batch:(k + 1) * batch]
            for k in range(drafts):
                o_logp[k:k + 1, :] = logp[:, k * batch:(k + 1) * batch]
            for pd, pt, dy, k in peers:
                s_copy(pd, pt, dy, k, slot).wait_send()

        hbm = pl.BlockSpec(memory_space=pl.ANY)
        vmem = pl.BlockSpec(memory_space=pltpu.VMEM)
        dma = pltpu.SemaphoreType.DMA
        bf16 = jnp.bfloat16
        logp, logn, ent = pl.pallas_call(
            kernel,
            out_shape=[jax.ShapeDtypeStruct((drafts, batch), f32), jax.ShapeDtypeStruct((pos, batch), f32),
                       jax.ShapeDtypeStruct((pos, batch), f32)],
            in_specs=[hbm] * 4,
            out_specs=[vmem] * 3,
            scratch_shapes=[
                pltpu.VMEM((tiles, half, TILE), bf16),
                pltpu.VMEM((rows, dim), bf16),
                pltpu.VMEM((2 * LANES, dim), bf16),
                pltpu.VMEM((parts, rows, LANES), f32),
                pltpu.VMEM((kblocks, rows, LANES), f32),
                pltpu.VMEM((half, 2 * LANES), f32),
                pltpu.VMEM((kblocks, LANES), bf16),
                pltpu.VMEM((kblocks, LANES), f32),
                pltpu.VMEM((drafts, batch), jnp.int32),
                pltpu.VMEM((drafts, batch), jnp.int32),
                pltpu.VMEM((2, 8, LANES), f32),
                pltpu.VMEM((2 * tp, 8, LANES), f32),
                dma((tiles,)),
                dma((3,)),
                dma((parts,)), dma((parts,)),
                dma((parts,)), dma((parts,)),
                dma((parts,)), dma((parts,)),
                dma((parts,)), dma((parts,)),
                dma, dma,
                dma((2 * tp,)), dma((2 * tp,)),
            ],
            compiler_params=pltpu.CompilerParams(
                collective_id=0, has_side_effects=True, vmem_limit_bytes=62 * 1024 * 1024),
        )(hidden.transpose(1, 0, 2).reshape(rows, dim), draft_ids.T, norm_gain.reshape(kblocks, LANES), head_w.T)
        return logp.T, logn.T, ent.T

    specs_in = (P('dp', None, None), P('dp', None), P(None), P(None, 'tp'))
    specs_out = (P('dp', None), P('dp', None), P('dp', None))
    return jax.shard_map(per_device, mesh=mesh, in_specs=specs_in, out_specs=specs_out, check_vma=False)
```

```python
import jax
import jax.numpy as jnp
from jax import lax
from jax.experimental import pallas as pl
from jax.experimental.pallas import tpu as pltpu
from jax.sharding import PartitionSpec as P

NORM_EPS = 1e-5
MESH = pl.DeviceIdType.MESH
LANES = 128
TILE = 256
BLOCK = 800
OWN = 1600
CHUNK = 400
AHEAD = 2
DEPTH = 4
NT = (((1,), (1,)), ((), ()))


def rows_sum(block):
    return jnp.sum(block.reshape(-1, 8, block.shape[-1]), axis=0)


def rows_max(block):
    return jnp.max(block.reshape(-1, 8, block.shape[-1]), axis=0)


def update_stats(z, row_ids, ids, carry, first=None):
    bm = rows_max(z)
    z3 = z.reshape(-1, 8, z.shape[-1])
    picked = rows_sum(jnp.where(row_ids == ids, z, 0.0))
    if carry is None:
        sh = z3 - bm[None]
        e = jnp.exp(sh)
        return bm, jnp.sum(e, axis=0), jnp.sum(e * sh, axis=0), picked
    m, s, w, p = carry
    if first is not None:
        m = jnp.where(first, bm, m)
    mn = jnp.maximum(m, bm)
    dm = m - mn
    a = jnp.exp(dm)
    sh = z3 - mn[None]
    e = jnp.exp(sh)
    w = a * (w + dm * s) + jnp.sum(e * sh, axis=0)
    s = a * s + jnp.sum(e, axis=0)
    return mn, s, w, p + picked


def merge_stats(a, b):
    top = jnp.maximum(a[0], b[0])
    da, db = a[0] - top, b[0] - top
    fa, fb = jnp.exp(da), jnp.exp(db)
    return (
        top,
        fa * a[1] + fb * b[1],
        fa * (a[2] + da * a[1]) + fb * (b[2] + db * b[1]),
        a[3] + b[3],
    )


def pack_stats(carry):
    m, s, w, p = carry
    top = jnp.max(m, axis=0, keepdims=True)
    dm = m - top
    f = jnp.exp(dm)
    return (
        top,
        jnp.sum(f * s, axis=0, keepdims=True),
        jnp.sum(f * (w + dm * s), axis=0, keepdims=True),
        jnp.sum(p, axis=0, keepdims=True),
    )


def solution(mesh):
    tp = mesh.shape['tp']

    def per_device(hidden, draft_ids, norm_gain, head_w):
        batch, pos, dim = hidden.shape
        drafts = draft_ids.shape[1]
        cols = head_w.shape[1]
        half = (cols - OWN) // 2
        chunks = OWN // CHUNK
        rows = batch * pos
        kblocks = dim // LANES
        tiles = dim // TILE
        parts = kblocks // tp
        ptiles = tiles // tp
        nblocks = half // BLOCK
        f32 = jnp.float32

        def kernel(x_hbm, ids_hbm, g_hbm, w_hbm, out,
                   ev, wv, xv, nb, nf, pf, acc, gv, gf, idv, idp, st, rs,
                   esem, wsem, lsem, ysend, yrecv, xsend, xrecv, asend, arecv, bsend, brecv, isend, irecv, ssem, rsem):
            t = lax.axis_index('tp')
            d = lax.axis_index('dp')
            y = lax.rem(d, 2)
            core = lax.rem(t, 2)
            mate = (d + 1 - 2 * y, t)
            sib = (d, t + 1 - 2 * core)
            nbr_t = lax.rem(t + 2, tp)
            nbr = (d, nbr_t)
            sib_t = t + 1 - 2 * core
            far_t = lax.rem(sib_t + 2, tp)

            cx = pltpu.make_async_copy(x_hbm, xv, lsem.at[0])
            cg = pltpu.make_async_copy(g_hbm, gv, lsem.at[1])
            ci = pltpu.make_async_copy(ids_hbm, idv, lsem.at[2])
            cx.start()
            cg.start()
            ci.start()

            def w_copy(kt):
                return pltpu.make_async_copy(
                    w_hbm.at[pl.ds(pl.multiple_of(OWN + y * half, 16), half), pl.ds(pl.multiple_of(kt * TILE, TILE), TILE)],
                    wv.at[kt], wsem.at[kt])

            def tile_of(stream_t, i):
                return stream_t * ptiles + i

            def plan(p):
                k = p // 2
                first = lax.rem(p, 2) == 0
                late = jnp.where(first, k - 2, k - 1)
                early_t = tile_of(jnp.where(first, t, sib_t), k)
                late_t = tile_of(jnp.where(first, far_t, nbr_t), late)
                return k, late, early_t, late_t, k < ptiles, (late >= 0) & (late < ptiles)

            def w_start(p):
                _, _, early_t, late_t, early_on, late_on = plan(p)

                @pl.when(early_on)
                def _():
                    w_copy(early_t).start()

                @pl.when(late_on)
                def _():
                    w_copy(late_t).start()

            def e_copy(e):
                return pltpu.make_async_copy(
                    w_hbm.at[pl.ds(pl.multiple_of(e * CHUNK, 16), CHUNK), :], ev.at[e], esem.at[e])

            e_copy(0).start()
            barrier = pltpu.get_barrier_semaphore()
            peers = []
            for dy in range(2):
                for k in range(tp):
                    if dy or k:
                        peers.append((mate[0] if dy else d, lax.rem(t + k, tp), dy, k))
            for pd, pt, _, _ in peers:
                pl.semaphore_signal(barrier, inc=1, device_id=(pd, pt), device_id_type=MESH)

            def y_copy(i):
                return pltpu.make_async_remote_copy(
                    src_ref=nf.at[i], dst_ref=pf.at[t * parts + i], send_sem=ysend.at[i], recv_sem=yrecv.at[i],
                    device_id=mate, device_id_type=MESH)

            def x_copy(i, owner):
                kb = owner * parts + i
                return pltpu.make_async_remote_copy(
                    src_ref=pf.at[kb], dst_ref=pf.at[kb], send_sem=xsend.at[i], recv_sem=xrecv.at[i],
                    device_id=nbr, device_id_type=MESH)

            def a_copy(i, owner):
                kb = owner * parts + i
                return pltpu.make_async_remote_copy(
                    src_ref=pf.at[kb], dst_ref=pf.at[kb], send_sem=asend.at[i], recv_sem=arecv.at[i],
                    device_id=sib, device_id_type=MESH)

            def b_copy(i, owner):
                kb = owner * parts + i
                return pltpu.make_async_remote_copy(
                    src_ref=pf.at[kb], dst_ref=pf.at[kb], send_sem=bsend.at[i], recv_sem=brecv.at[i],
                    device_id=sib, device_id_type=MESH)

            id_copy = pltpu.make_async_remote_copy(
                src_ref=idv, dst_ref=idp, send_sem=isend, recv_sem=irecv, device_id=mate, device_id_type=MESH)

            nb[rows:LANES, :] = jnp.zeros((LANES - rows, dim), jnp.bfloat16)
            nb[LANES + rows:, :] = jnp.zeros((LANES - rows, dim), jnp.bfloat16)
            with jax.named_scope('waitg'):
                ci.wait()
                cg.wait()
            gf[...] = gv[...].astype(f32)
            with jax.named_scope('waitx'):
                cx.wait()
            e_copy(1).start()
            sq = jnp.zeros((rows, LANES), f32)
            for k in range(kblocks):
                x = xv[:, k * LANES:(k + 1) * LANES].astype(f32)
                sq = sq + x * x
            inv = lax.rsqrt(jnp.sum(sq, axis=1, keepdims=True) / dim + NORM_EPS)

            def normed(kb):
                x = xv[:, pl.ds(pl.multiple_of(kb * LANES, LANES), LANES)].astype(f32)
                return (x * inv * gf[pl.ds(kb, 1), :]).astype(jnp.bfloat16)

            for i in range(parts):
                nf[i] = normed(t * parts + i).astype(f32)
            with jax.named_scope('barr'):
                pl.semaphore_wait(barrier, len(peers))
            for i in range(parts):
                y_copy(i).start()
            id_copy.start()
            for k in range(kblocks):
                nb[:rows, k * LANES:(k + 1) * LANES] = normed(k)
            acc[...] = jnp.zeros_like(acc)

            def forward_y(i):
                y_copy(i).wait_recv()
                x_copy(i, t).start()
                a_copy(i, t).start()

            def forward_x(i):
                x_copy(i, nbr_t).wait_recv()
                b_copy(i, nbr_t).start()

            def load_tile(kt):
                with jax.named_scope('ww'):
                    w_copy(kt).wait()
                for h in range(2):
                    nb[LANES:LANES + rows, pl.ds(pl.multiple_of(kt * TILE + h * LANES, LANES), LANES)] = (
                        pf[2 * kt + h].astype(jnp.bfloat16))

            def tile_dot(kt, r):
                return lax.dot_general(wv[kt, r, :], nb[:, pl.ds(pl.multiple_of(kt * TILE, TILE), TILE)], NT,
                                       preferred_element_type=f32)

            own_ids = jnp.concatenate([idv[k:k + 1, :] for k in range(drafts)]
                                      + [jnp.full((1, LANES - drafts * batch), -1, jnp.int32)], axis=1) - t * cols
            own_iota = lax.broadcasted_iota(jnp.int32, (CHUNK, LANES), 0)

            def own_step(e, carry):
                with jax.named_scope('waite'):
                    e_copy(e).wait()

                @pl.when(e + 2 < chunks)
                def _():
                    e_copy(e + 2).start()

                @pl.when(e == chunks - 2)
                def _():
                    w_start(0)
                    w_start(1)

                @pl.when(e == chunks - 1)
                def _():
                    w_start(2)
                    w_start(3)

                with jax.named_scope('own'):
                    z = lax.dot_general(ev[e], nb[:LANES, :], NT, preferred_element_type=f32)
                    carry = update_stats(z, own_iota, own_ids - e * CHUNK, carry, e == 0)

                @pl.when(e >= chunks - AHEAD)
                def _():
                    with jax.named_scope('fyo'):
                        forward_y(e - (chunks - AHEAD))

                return carry

            zero = jnp.zeros((8, LANES), f32)
            own_carry = lax.fori_loop(0, chunks, own_step, (zero, zero, zero, zero))

            last_p = 2 * ptiles + 2

            def step(p, _):
                k, late, early_t, late_t, early_on, late_on = plan(p)

                @pl.when(p + DEPTH <= last_p)
                def _():
                    w_start(p + DEPTH)

                @pl.when(p + AHEAD < parts)
                def _():
                    with jax.named_scope('fy'):
                        forward_y(p + AHEAD)

                @pl.when((p >= 2) & (p - 2 < parts))
                def _():
                    with jax.named_scope('fx'):
                        forward_x(p - 2)

                @pl.when((p % 2 == 1) & early_on)
                def _():
                    with jax.named_scope('wa'):
                        a_copy(2 * k, sib_t).wait_recv()
                        a_copy(2 * k + 1, sib_t).wait_recv()

                @pl.when((p % 2 == 0) & late_on)
                def _():
                    with jax.named_scope('wb'):
                        b_copy(2 * late, far_t).wait_recv()
                        b_copy(2 * late + 1, far_t).wait_recv()

                @pl.when(early_on & late_on)
                def _():
                    load_tile(early_t)
                    load_tile(late_t)
                    with jax.named_scope('dual'):
                        for n in range(nblocks):
                            r = slice(n * BLOCK, (n + 1) * BLOCK)
                            acc[r, :] = acc[r, :] + (tile_dot(early_t, r) + tile_dot(late_t, r))

                @pl.when(jnp.logical_not(early_on & late_on))
                def _():
                    one = jnp.where(early_on, early_t, late_t)
                    load_tile(one)
                    with jax.named_scope('single'):
                        for n in range(nblocks):
                            r = slice(n * BLOCK, (n + 1) * BLOCK)
                            acc[r, :] = acc[r, :] + tile_dot(one, r)

                return 0

            lax.fori_loop(0, last_p, step, 0)

            pad = jnp.full((1, LANES - drafts * batch), -1, jnp.int32)
            id_copy.wait_recv()
            ids = jnp.concatenate([idv[k:k + 1, :] for k in range(drafts)] + [pad]
                                  + [idp[k:k + 1, :] for k in range(drafts)] + [pad], axis=1)
            ids = ids - (t * cols + OWN + y * half)
            row_iota = lax.broadcasted_iota(jnp.int32, (BLOCK, TILE), 0)
            last_t = tile_of(far_t, ptiles - 1)
            with jax.named_scope('wlast'):
                b_copy(parts - 2, far_t).wait_recv()
                b_copy(parts - 1, far_t).wait_recv()
            load_tile(last_t)
            carry = None
            with jax.named_scope('final'):
                for n in range(nblocks):
                    r = slice(n * BLOCK, (n + 1) * BLOCK)
                    z = acc[r, :] + tile_dot(last_t, r)
                    carry = update_stats(z, row_iota, ids - n * BLOCK, carry)
            mine = pack_stats(merge_stats(own_carry, [c[:, :LANES] for c in carry]))
            theirs = pack_stats([c[:, LANES:] for c in carry])
            slot = y * tp + t
            for k in range(4):
                st[0, k:k + 1, :] = mine[k]
                st[1, k:k + 1, :] = theirs[k]
                rs[slot, k:k + 1, :] = mine[k]

            def s_copy(pd, pt, dy, k, into):
                return pltpu.make_async_remote_copy(
                    src_ref=st.at[dy], dst_ref=rs.at[into], send_sem=ssem.at[dy * tp + k], recv_sem=rsem.at[into],
                    device_id=(pd, pt), device_id_type=MESH)

            for pd, pt, dy, k in peers:
                s_copy(pd, pt, dy, k, slot).start()
            for i in range(parts):
                y_copy(i).wait_send()
                x_copy(i, t).wait_send()
                a_copy(i, t).wait_send()
                b_copy(i, nbr_t).wait_send()
            id_copy.wait_send()
            with jax.named_scope('wstat'):
                for pd, pt, dy, k in peers:
                    s_copy(pd, pt, dy, k, (1 - y if dy else y) * tp + pt).wait_recv()
            ms = [rs[k, 0:1, :] for k in range(2 * tp)]
            top = ms[0]
            for k in range(1, 2 * tp):
                top = jnp.maximum(top, ms[k])
            s = jnp.zeros((1, LANES), f32)
            w = s
            p = s
            for k in range(2 * tp):
                dm = ms[k] - top
                f = jnp.exp(dm)
                s = s + f * rs[k, 1:2, :]
                w = w + f * (rs[k, 2:3, :] + dm * rs[k, 1:2, :])
                p = p + rs[k, 3:4, :]
            log_sum = jnp.log(s)
            log_norm = top + log_sum
            ent = log_sum - w / s
            logp = p - log_norm
            for k in range(pos):
                out[k:k + 1, :] = log_norm[:, k * batch:(k + 1) * batch]
                out[pos + k:pos + k + 1, :] = ent[:, k * batch:(k + 1) * batch]
                out[2 * pos + k:2 * pos + k + 1, :] = logp[:, k * batch:(k + 1) * batch]
            for pd, pt, dy, k in peers:
                s_copy(pd, pt, dy, k, slot).wait_send()

        hbm = pl.BlockSpec(memory_space=pl.ANY)
        vmem = pl.BlockSpec(memory_space=pltpu.VMEM)
        dma = pltpu.SemaphoreType.DMA
        bf16 = jnp.bfloat16
        packed = pl.pallas_call(
            kernel,
            out_shape=jax.ShapeDtypeStruct((3 * pos, batch), f32),
            in_specs=[hbm] * 4,
            out_specs=vmem,
            scratch_shapes=[
                pltpu.VMEM((chunks, CHUNK, dim), bf16),
                pltpu.VMEM((tiles, half, TILE), bf16),
                pltpu.VMEM((rows, dim), bf16),
                pltpu.VMEM((2 * LANES, dim), bf16),
                pltpu.VMEM((parts, rows, LANES), f32),
                pltpu.VMEM((kblocks, rows, LANES), f32),
                pltpu.VMEM((half, 2 * LANES), f32),
                pltpu.VMEM((kblocks, LANES), bf16),
                pltpu.VMEM((kblocks, LANES), f32),
                pltpu.VMEM((drafts, batch), jnp.int32),
                pltpu.VMEM((drafts, batch), jnp.int32),
                pltpu.VMEM((2, 8, LANES), f32),
                pltpu.VMEM((2 * tp, 8, LANES), f32),
                dma((chunks,)),
                dma((tiles,)),
                dma((3,)),
                dma((parts,)), dma((parts,)),
                dma((parts,)), dma((parts,)),
                dma((parts,)), dma((parts,)),
                dma((parts,)), dma((parts,)),
                dma, dma,
                dma((2 * tp,)), dma((2 * tp,)),
            ],
            compiler_params=pltpu.CompilerParams(
                collective_id=0, has_side_effects=True, vmem_limit_bytes=60 * 1024 * 1024),
        )(hidden.transpose(1, 0, 2).reshape(rows, dim), draft_ids.T, norm_gain.reshape(kblocks, LANES), head_w.T)

        def split(src, o_logp, o_logn, o_ent):
            o_logn[...] = src[:pos, :]
            o_ent[...] = src[pos:2 * pos, :]
            o_logp[...] = src[2 * pos:2 * pos + drafts, :]

        logp, logn, ent = pl.pallas_call(
            split,
            out_shape=[jax.ShapeDtypeStruct((drafts, batch), f32), jax.ShapeDtypeStruct((pos, batch), f32),
                       jax.ShapeDtypeStruct((pos, batch), f32)],
            in_specs=[vmem],
            out_specs=[vmem] * 3,
        )(packed)
        return logp.T, logn.T, ent.T

    specs_in = (P('dp', None, None), P('dp', None), P(None), P(None, 'tp'))
    specs_out = (P('dp', None), P('dp', None), P('dp', None))
    return jax.shard_map(per_device, mesh=mesh, in_specs=specs_in, out_specs=specs_out, check_vma=False)
```

```python
import jax
import jax.numpy as jnp
from jax import lax
from jax.experimental import pallas as pl
from jax.experimental.pallas import tpu as pltpu
from jax.sharding import PartitionSpec as P

NORM_EPS = 1e-5
MESH = pl.DeviceIdType.MESH
LANES = 128
TILE = 256
BLOCK = 800
OWN = 1600
CHUNK = 400
DEPTH = 6
OWN_FORWARDS = ((), (0,), (1, 2), (3,))
STEPS = (
    ((), (), ('y0', 'y1')),
    ((4,), (0,), ('a0', 'a1')),
    ((5, 6), (1, 2), ('x0', 'y2')),
    ((7,), (3,), ('b0', 'a2', 'x1')),
    ((8, 9), (4,), ('y3', 'y4', 'a3', 'b1')),
    ((), (5, 6, 7), ('x2', 'x3', 'a4')),
    ((), (8, 9), ('b2', 'b3', 'x4')),
    ((), (), ('b4',)),
)
NT = (((1,), (1,)), ((), ()))


def rows_sum(block):
    return jnp.sum(block.reshape(-1, 8, block.shape[-1]), axis=0)


def rows_max(block):
    return jnp.max(block.reshape(-1, 8, block.shape[-1]), axis=0)


def update_stats(z, row_ids, ids, carry, first=None):
    bm = rows_max(z)
    z3 = z.reshape(-1, 8, z.shape[-1])
    picked = rows_sum(jnp.where(row_ids == ids, z, 0.0))
    if carry is None:
        sh = z3 - bm[None]
        e = jnp.exp(sh)
        return bm, jnp.sum(e, axis=0), jnp.sum(e * sh, axis=0), picked
    m, s, w, p = carry
    if first is not None:
        m = jnp.where(first, bm, m)
    mn = jnp.maximum(m, bm)
    dm = m - mn
    a = jnp.exp(dm)
    sh = z3 - mn[None]
    e = jnp.exp(sh)
    w = a * (w + dm * s) + jnp.sum(e * sh, axis=0)
    s = a * s + jnp.sum(e, axis=0)
    return mn, s, w, p + picked


def merge_stats(a, b):
    top = jnp.maximum(a[0], b[0])
    da, db = a[0] - top, b[0] - top
    fa, fb = jnp.exp(da), jnp.exp(db)
    return (
        top,
        fa * a[1] + fb * b[1],
        fa * (a[2] + da * a[1]) + fb * (b[2] + db * b[1]),
        a[3] + b[3],
    )


def pack_stats(carry):
    m, s, w, p = carry
    top = jnp.max(m, axis=0, keepdims=True)
    dm = m - top
    f = jnp.exp(dm)
    return (
        top,
        jnp.sum(f * s, axis=0, keepdims=True),
        jnp.sum(f * (w + dm * s), axis=0, keepdims=True),
        jnp.sum(p, axis=0, keepdims=True),
    )


def solution(mesh):
    tp = mesh.shape['tp']

    def per_device(hidden, draft_ids, norm_gain, head_w):
        batch, pos, dim = hidden.shape
        drafts = draft_ids.shape[1]
        cols = head_w.shape[1]
        half = (cols - OWN) // 2
        chunks = OWN // CHUNK
        rows = batch * pos
        kblocks = dim // LANES
        tiles = dim // TILE
        parts = kblocks // tp
        ptiles = tiles // tp
        nblocks = half // BLOCK
        f32 = jnp.float32

        def kernel(x_hbm, ids_hbm, g_hbm, w_hbm, out,
                   ev, wv, xv, nb, nf, pf, acc, gv, gf, idv, idp, st, rs,
                   esem, wsem, lsem, ysend, yrecv, xsend, xrecv, asend, arecv, bsend, brecv, isend, irecv, ssem, rsem):
            t = lax.axis_index('tp')
            d = lax.axis_index('dp')
            y = lax.rem(d, 2)
            core = lax.rem(t, 2)
            mate = (d + 1 - 2 * y, t)
            sib = (d, t + 1 - 2 * core)
            nbr_t = lax.rem(t + 2, tp)
            nbr = (d, nbr_t)
            sib_t = t + 1 - 2 * core
            far_t = lax.rem(sib_t + 2, tp)

            cx = pltpu.make_async_copy(x_hbm, xv, lsem.at[0])
            cg = pltpu.make_async_copy(g_hbm, gv, lsem.at[1])
            ci = pltpu.make_async_copy(ids_hbm, idv, lsem.at[2])
            cx.start()
            cg.start()
            ci.start()

            def w_copy(kt):
                return pltpu.make_async_copy(
                    w_hbm.at[pl.ds(pl.multiple_of(OWN + y * half, 16), half), pl.ds(pl.multiple_of(kt * TILE, TILE), TILE)],
                    wv.at[kt], wsem.at[kt])

            def tile_of(stream_t, i):
                return stream_t * ptiles + i

            stream_t = {'y': t, 'a': sib_t, 'x': nbr_t, 'b': far_t}

            def kt_of(name):
                return tile_of(stream_t[name[0]], int(name[1:]))

            order = [name for _, _, names in STEPS for name in names]

            def e_copy(e):
                return pltpu.make_async_copy(
                    w_hbm.at[pl.ds(pl.multiple_of(e * CHUNK, 16), CHUNK), :], ev.at[e], esem.at[e])

            e_copy(0).start()
            barrier = pltpu.get_barrier_semaphore()
            peers = []
            for dy in range(2):
                for k in range(tp):
                    if dy or k:
                        peers.append((mate[0] if dy else d, lax.rem(t + k, tp), dy, k))
            for pd, pt, _, _ in peers:
                pl.semaphore_signal(barrier, inc=1, device_id=(pd, pt), device_id_type=MESH)

            def y_copy(i):
                return pltpu.make_async_remote_copy(
                    src_ref=nf.at[i], dst_ref=pf.at[t * parts + i], send_sem=ysend, recv_sem=yrecv.at[i],
                    device_id=mate, device_id_type=MESH)

            def x_copy(i, owner):
                kb = owner * parts + i
                return pltpu.make_async_remote_copy(
                    src_ref=pf.at[kb], dst_ref=pf.at[kb], send_sem=xsend, recv_sem=xrecv.at[i],
                    device_id=nbr, device_id_type=MESH)

            def a_copy(i, owner):
                kb = owner * parts + i
                return pltpu.make_async_remote_copy(
                    src_ref=pf.at[kb], dst_ref=pf.at[kb], send_sem=asend, recv_sem=arecv.at[i],
                    device_id=sib, device_id_type=MESH)

            def b_copy(i, owner):
                kb = owner * parts + i
                return pltpu.make_async_remote_copy(
                    src_ref=pf.at[kb], dst_ref=pf.at[kb], send_sem=bsend, recv_sem=brecv.at[i],
                    device_id=sib, device_id_type=MESH)

            id_copy = pltpu.make_async_remote_copy(
                src_ref=idv, dst_ref=idp, send_sem=isend, recv_sem=irecv, device_id=mate, device_id_type=MESH)

            nb[rows:LANES, :] = jnp.zeros((LANES - rows, dim), jnp.bfloat16)
            nb[LANES + rows:, :] = jnp.zeros((LANES - rows, dim), jnp.bfloat16)
            with jax.named_scope('waitg'):
                ci.wait()
                cg.wait()
            gf[...] = gv[...].astype(f32)
            with jax.named_scope('waitx'):
                cx.wait()
            e_copy(1).start()
            sq = jnp.zeros((rows, LANES), f32)
            for k in range(kblocks):
                x = xv[:, k * LANES:(k + 1) * LANES].astype(f32)
                sq = sq + x * x
            inv = lax.rsqrt(jnp.sum(sq, axis=1, keepdims=True) / dim + NORM_EPS)

            def normed(kb):
                x = xv[:, pl.ds(pl.multiple_of(kb * LANES, LANES), LANES)].astype(f32)
                return (x * inv * gf[pl.ds(kb, 1), :]).astype(jnp.bfloat16)

            for i in range(parts):
                nf[i] = normed(t * parts + i).astype(f32)
            with jax.named_scope('barr'):
                pl.semaphore_wait(barrier, len(peers))
            for i in range(parts):
                y_copy(i).start()
            id_copy.start()
            for k in range(kblocks):
                nb[:rows, k * LANES:(k + 1) * LANES] = normed(k)

            def forward_y(i):
                y_copy(i).wait_recv()
                x_copy(i, t).start()
                a_copy(i, t).start()

            def forward_x(i):
                x_copy(i, nbr_t).wait_recv()
                b_copy(i, nbr_t).start()

            def load_tile(name):
                kt = kt_of(name)
                nxt = order.index(name) + DEPTH
                if nxt < len(order):
                    w_copy(kt_of(order[nxt])).start()
                i = int(name[1:])
                with jax.named_scope('wait_' + name):
                    for h in range(2):
                        if name[0] == 'a':
                            a_copy(2 * i + h, sib_t).wait_recv()
                        if name[0] == 'b':
                            b_copy(2 * i + h, far_t).wait_recv()
                with jax.named_scope('ww'):
                    w_copy(kt).wait()
                for h in range(2):
                    nb[LANES:LANES + rows, pl.ds(pl.multiple_of(kt * TILE + h * LANES, LANES), LANES)] = (
                        pf[2 * kt + h].astype(jnp.bfloat16))

            def tiles_dot(names, r):
                z = None
                for name in names:
                    kt = kt_of(name)
                    one = lax.dot_general(wv[kt, r, :], nb[:, pl.ds(pl.multiple_of(kt * TILE, TILE), TILE)], NT,
                                          preferred_element_type=f32)
                    z = one if z is None else z + one
                return z

            own_ids = jnp.concatenate([idv[k:k + 1, :] for k in range(drafts)]
                                      + [jnp.full((1, LANES - drafts * batch), -1, jnp.int32)], axis=1) - t * cols
            own_iota = lax.broadcasted_iota(jnp.int32, (CHUNK, LANES), 0)

            def own_step(e, carry):
                with jax.named_scope('waite'):
                    e_copy(e).wait()

                @pl.when(e + 2 < chunks)
                def _():
                    e_copy(e + 2).start()

                @pl.when(e == chunks - 2)
                def _():
                    for name in order[:DEPTH // 2]:
                        w_copy(kt_of(name)).start()

                @pl.when(e == chunks - 1)
                def _():
                    for name in order[DEPTH // 2:DEPTH]:
                        w_copy(kt_of(name)).start()

                with jax.named_scope('own'):
                    z = lax.dot_general(ev[e], nb[:LANES, :], NT, preferred_element_type=f32)
                    carry = update_stats(z, own_iota, own_ids - e * CHUNK, carry, e == 0)
                for chunk, blocks in enumerate(OWN_FORWARDS):
                    if blocks:
                        @pl.when(e == chunk)
                        def _():
                            with jax.named_scope('fy'):
                                for i in blocks:
                                    forward_y(i)
                return carry

            zero = jnp.zeros((8, LANES), f32)
            own_carry = lax.fori_loop(0, chunks, own_step, (zero, zero, zero, zero))

            for n_step, (ys, xs, names) in enumerate(STEPS[:-1]):
                for i in ys:
                    with jax.named_scope('fy'):
                        forward_y(i)
                for i in xs:
                    with jax.named_scope('fx'):
                        forward_x(i)
                for name in names:
                    load_tile(name)

                @pl.when(t >= 0)
                def _():
                    with jax.named_scope('step'):
                        for n in range(nblocks):
                            r = slice(n * BLOCK, (n + 1) * BLOCK)
                            z = tiles_dot(names, r)
                            acc[r, :] = z if n_step == 0 else acc[r, :] + z

            pad = jnp.full((1, LANES - drafts * batch), -1, jnp.int32)
            id_copy.wait_recv()
            ids = jnp.concatenate([idv[k:k + 1, :] for k in range(drafts)] + [pad]
                                  + [idp[k:k + 1, :] for k in range(drafts)] + [pad], axis=1)
            ids = ids - (t * cols + OWN + y * half)
            row_iota = lax.broadcasted_iota(jnp.int32, (BLOCK, TILE), 0)
            load_tile(order[-1])
            carry = None
            with jax.named_scope('final'):
                for n in range(nblocks):
                    r = slice(n * BLOCK, (n + 1) * BLOCK)
                    z = acc[r, :] + tiles_dot(order[-1:], r)
                    carry = update_stats(z, row_iota, ids - n * BLOCK, carry)
            mine = pack_stats(merge_stats(own_carry, [c[:, :LANES] for c in carry]))
            theirs = pack_stats([c[:, LANES:] for c in carry])
            slot = y * tp + t
            for k in range(4):
                st[0, k:k + 1, :] = mine[k]
                st[1, k:k + 1, :] = theirs[k]
                rs[slot, k:k + 1, :] = mine[k]

            def s_copy(pd, pt, dy, k, into):
                return pltpu.make_async_remote_copy(
                    src_ref=st.at[dy], dst_ref=rs.at[into], send_sem=ssem, recv_sem=rsem.at[into],
                    device_id=(pd, pt), device_id_type=MESH)

            for pd, pt, dy, k in peers:
                s_copy(pd, pt, dy, k, slot).start()
            for sem in (ysend, xsend, asend, bsend):
                pltpu.make_async_remote_copy(
                    src_ref=nf, dst_ref=nf, send_sem=sem, recv_sem=irecv, device_id=sib, device_id_type=MESH).wait_send()
            id_copy.wait_send()
            with jax.named_scope('wstat'):
                for pd, pt, dy, k in peers:
                    s_copy(pd, pt, dy, k, (1 - y if dy else y) * tp + pt).wait_recv()
            with jax.named_scope('combine'):
                ms = [rs[k, 0:1, :] for k in range(2 * tp)]
                top = ms[0]
                for k in range(1, 2 * tp):
                    top = jnp.maximum(top, ms[k])
                s = jnp.zeros((1, LANES), f32)
                w = s
                p = s
                for k in range(2 * tp):
                    dm = ms[k] - top
                    f = jnp.exp(dm)
                    s = s + f * rs[k, 1:2, :]
                    w = w + f * (rs[k, 2:3, :] + dm * rs[k, 1:2, :])
                    p = p + rs[k, 3:4, :]
                log_sum = jnp.log(s)
                log_norm = top + log_sum
                ent = log_sum - w / s
                logp = p - log_norm
                for k in range(pos):
                    out[k:k + 1, :] = log_norm[:, k * batch:(k + 1) * batch]
                    out[pos + k:pos + k + 1, :] = ent[:, k * batch:(k + 1) * batch]
                    out[2 * pos + k:2 * pos + k + 1, :] = logp[:, k * batch:(k + 1) * batch]
            with jax.named_scope('wsend'):
                every = rs.at[pl.ds(0, len(peers))]
                pltpu.make_async_remote_copy(
                    src_ref=every, dst_ref=every, send_sem=ssem, recv_sem=irecv, device_id=sib, device_id_type=MESH).wait_send()

        hbm = pl.BlockSpec(memory_space=pl.ANY)
        vmem = pl.BlockSpec(memory_space=pltpu.VMEM)
        dma = pltpu.SemaphoreType.DMA
        bf16 = jnp.bfloat16
        packed = pl.pallas_call(
            kernel,
            out_shape=pltpu.VMEM((3 * pos, batch), f32),
            in_specs=[hbm] * 4,
            out_specs=vmem,
            scratch_shapes=[
                pltpu.VMEM((chunks, CHUNK, dim), bf16),
                pltpu.VMEM((tiles, half, TILE), bf16),
                pltpu.VMEM((rows, dim), bf16),
                pltpu.VMEM((2 * LANES, dim), bf16),
                pltpu.VMEM((parts, rows, LANES), f32),
                pltpu.VMEM((kblocks, rows, LANES), f32),
                pltpu.VMEM((half, 2 * LANES), f32),
                pltpu.VMEM((kblocks, LANES), bf16),
                pltpu.VMEM((kblocks, LANES), f32),
                pltpu.VMEM((drafts, batch), jnp.int32),
                pltpu.VMEM((drafts, batch), jnp.int32),
                pltpu.VMEM((2, 8, LANES), f32),
                pltpu.VMEM((2 * tp, 8, LANES), f32),
                dma((chunks,)),
                dma((tiles,)),
                dma((3,)),
                dma, dma((parts,)),
                dma, dma((parts,)),
                dma, dma((parts,)),
                dma, dma((parts,)),
                dma, dma,
                dma, dma((2 * tp,)),
            ],
            compiler_params=pltpu.CompilerParams(
                collective_id=0, has_side_effects=True, vmem_limit_bytes=60 * 1024 * 1024),
        )(hidden.transpose(1, 0, 2).reshape(rows, dim), draft_ids.T, norm_gain.reshape(kblocks, LANES), head_w.T)

        def split(src, o_logp, o_logn, o_ent):
            o_logn[...] = src[:pos, :]
            o_ent[...] = src[pos:2 * pos, :]
            o_logp[...] = src[2 * pos:2 * pos + drafts, :]

        logp, logn, ent = pl.pallas_call(
            split,
            out_shape=[jax.ShapeDtypeStruct((drafts, batch), f32), jax.ShapeDtypeStruct((pos, batch), f32),
                       jax.ShapeDtypeStruct((pos, batch), f32)],
            in_specs=[vmem],
            out_specs=[vmem] * 3,
        )(pltpu.with_memory_space_constraint(packed, pltpu.VMEM))
        return logp.T, logn.T, ent.T

    specs_in = (P('dp', None, None), P('dp', None), P(None), P(None, 'tp'))
    specs_out = (P('dp', None), P('dp', None), P('dp', None))
    return jax.shard_map(per_device, mesh=mesh, in_specs=specs_in, out_specs=specs_out, check_vma=False)
```

```python
import jax
import jax.numpy as jnp
from jax import lax
from jax.experimental import pallas as pl
from jax.experimental.pallas import tpu as pltpu
from jax.sharding import PartitionSpec as P

NORM_EPS = 1e-5
MESH = pl.DeviceIdType.MESH
LANES = 128
TILE = 256
BLOCK = 800
OWN = 1600
FIRST = 160
CHUNK = 360
LAST = 320
DIRECT = 6
SHARED = 2
OWN_FORWARDS = ((), (0,), (1,), (2, 3))
STEPS = (
    ((), (), ('y0', 'y1', 'a0')),
    ((4, 5), (0,), ('a1', 'y2')),
    ((6,), (1,), ('x0', 'a2')),
    ((7,), (2, 3), ('y3', 'x1', 'b0')),
    ((8, 9), (4, 5), ('a3', 'b1', 'y4', 'x2')),
    ((10, 11), (6, 7), ('a4', 'b2', 'y5', 'x3')),
    ((), (), ('a5', 'b3')),
)
NT = (((1,), (1,)), ((), ()))


def update_stats(z, want, carry, first=None):
    z3 = z.reshape(-1, 8, z.shape[-1])
    bm = jnp.max(z3, axis=0)
    m, s, w, p = carry
    for g in range(z3.shape[0]):
        p = jnp.where(want == g, z3[g], p)
    if m is None:
        sh = z3 - bm[None]
        e = jnp.exp(sh)
        return bm, jnp.sum(e, axis=0), jnp.sum(e * sh, axis=0), p
    mn = jnp.maximum(m, bm)
    dm = m - mn
    a = jnp.exp(dm)
    sh = z3 - mn[None]
    e = jnp.exp(sh)
    w = a * (w + dm * s) + jnp.sum(e * sh, axis=0)
    s = a * s + jnp.sum(e, axis=0)
    return mn, s, w, p


def merge_stats(a, b):
    top = jnp.maximum(a[0], b[0])
    da, db = a[0] - top, b[0] - top
    fa, fb = jnp.exp(da), jnp.exp(db)
    return (
        top,
        fa * a[1] + fb * b[1],
        fa * (a[2] + da * a[1]) + fb * (b[2] + db * b[1]),
        a[3] + b[3],
    )


def keep_row(carry, ids):
    m, s, w, p = carry
    sub = lax.broadcasted_iota(jnp.int32, p.shape, 0)
    return m, s, w, jnp.where(sub == jnp.bitwise_and(ids, 7), p, 0.0)


def pack_stats(carry):
    m, s, w, p = carry
    top = jnp.max(m, axis=0, keepdims=True)
    dm = m - top
    f = jnp.exp(dm)
    return (
        top,
        jnp.sum(f * s, axis=0, keepdims=True),
        jnp.sum(f * (w + dm * s), axis=0, keepdims=True),
        jnp.sum(p, axis=0, keepdims=True),
    )


def solution(mesh):
    tp = mesh.shape['tp']

    def per_device(hidden, draft_ids, norm_gain, head_w):
        batch, pos, dim = hidden.shape
        drafts = draft_ids.shape[1]
        cols = head_w.shape[1]
        half = (cols - OWN) // 2
        chunks = (OWN - FIRST) // CHUNK
        rows = batch * pos
        kblocks = dim // LANES
        tiles = dim // TILE
        unique = DIRECT - SHARED
        assert tiles == tp * unique + 2 * SHARED
        parts = 2 * DIRECT
        crossing = 2 * unique
        nblocks = half // BLOCK
        f32 = jnp.float32

        def kernel(x_hbm, ids_hbm, g_hbm, w_hbm, out,
                   hv, ev, wv, xv, nb, nf, pf, acc, gv, gf, idv, idp, st, rs,
                   esem, wsem, lsem, ysend, yrecv, xsend, xrecv, asend, arecv, bsend, brecv, isend, irecv, ssem, rsem):
            t = lax.axis_index('tp')
            d = lax.axis_index('dp')
            y = lax.rem(d, 2)
            core = lax.rem(t, 2)
            mate = (d + 1 - 2 * y, t)
            sib = (d, t + 1 - 2 * core)
            nbr_t = lax.rem(t + 2, tp)
            nbr = (d, nbr_t)
            sib_t = t + 1 - 2 * core
            far_t = lax.rem(sib_t + 2, tp)

            cx = pltpu.make_async_copy(x_hbm, xv, lsem.at[0])
            cg = pltpu.make_async_copy(g_hbm, gv, lsem.at[1])
            ci = pltpu.make_async_copy(ids_hbm, idv, lsem.at[2])
            cg.start()
            ci.start()
            for k in range(pos):
                part = pl.ds(k * batch, batch)
                pltpu.make_async_copy(x_hbm.at[part], xv.at[part], lsem.at[0]).start()

            def w_copy(kt, group):
                return pltpu.make_async_copy(
                    w_hbm.at[pl.ds(pl.multiple_of(OWN + y * half, 16), half), pl.ds(pl.multiple_of(kt * TILE, TILE), TILE)],
                    wv.at[kt], wsem.at[group])

            def w_start(group):
                for name in STEPS[group][2]:
                    w_copy(kt_of(name), group).start()

            def w_wait(group):
                some = wv.at[pl.ds(0, len(STEPS[group][2]))]
                pltpu.make_async_copy(some, some, wsem.at[group]).wait()

            def tile_of(owner, i):
                if i < unique:
                    return owner * unique + i
                return tp * unique + lax.rem(owner, 2) * SHARED + i - unique

            def block_of(owner, i):
                return 2 * tile_of(owner, i // 2) + i % 2

            stream_t = {'y': t, 'a': sib_t, 'x': nbr_t, 'b': far_t}

            def kt_of(name):
                return tile_of(stream_t[name[0]], int(name[1:]))

            def e_copy(e):
                return pltpu.make_async_copy(
                    w_hbm.at[pl.ds(pl.multiple_of(FIRST + e * CHUNK, 8), CHUNK), :], ev.at[e], esem.at[lax.rem(e, 2)])

            head_copy = pltpu.make_async_copy(w_hbm.at[pl.ds(0, FIRST), :], hv, lsem.at[3])
            head_copy.start()
            e_copy(0).start()
            barrier = pltpu.get_barrier_semaphore()
            peers = []
            for dy in range(2):
                for k in range(tp):
                    if dy or k:
                        peers.append((mate[0] if dy else d, lax.rem(t + k, tp), dy, k))
            for near in (mate, sib, nbr):
                pl.semaphore_signal(barrier, inc=1, device_id=near, device_id_type=MESH)

            def y_copy(i):
                return pltpu.make_async_remote_copy(
                    src_ref=nf.at[i], dst_ref=pf.at[block_of(t, i)], send_sem=ysend, recv_sem=yrecv.at[i],
                    device_id=mate, device_id_type=MESH)

            def x_copy(i, owner):
                kb = block_of(owner, i)
                return pltpu.make_async_remote_copy(
                    src_ref=pf.at[kb], dst_ref=pf.at[kb], send_sem=xsend, recv_sem=xrecv.at[i],
                    device_id=nbr, device_id_type=MESH)

            def a_copy(i, owner):
                kb = block_of(owner, i)
                return pltpu.make_async_remote_copy(
                    src_ref=pf.at[kb], dst_ref=pf.at[kb], send_sem=asend, recv_sem=arecv.at[i // 2],
                    device_id=sib, device_id_type=MESH)

            def b_copy(i, owner):
                kb = block_of(owner, i)
                return pltpu.make_async_remote_copy(
                    src_ref=pf.at[kb], dst_ref=pf.at[kb], send_sem=bsend, recv_sem=brecv.at[i // 2],
                    device_id=sib, device_id_type=MESH)

            def tile_recv(owner, i, send, recv):
                both = pf.at[pl.ds(2 * tile_of(owner, i), 2)]
                pltpu.make_async_remote_copy(
                    src_ref=both, dst_ref=both, send_sem=send, recv_sem=recv.at[i],
                    device_id=sib, device_id_type=MESH).wait_recv()

            id_copy = pltpu.make_async_remote_copy(
                src_ref=idv, dst_ref=idp, send_sem=isend, recv_sem=irecv, device_id=mate, device_id_type=MESH)

            nb[rows:LANES, :] = jnp.zeros((LANES - rows, dim), jnp.bfloat16)
            nb[LANES + rows:, :] = jnp.zeros((LANES - rows, dim), jnp.bfloat16)
            with jax.named_scope('waitg'):
                ci.wait()
                cg.wait()
            gf[...] = gv[...].astype(f32)
            with jax.named_scope('waitx'):
                cx.wait()
            sq = jnp.zeros((rows, LANES), f32)
            for k in range(kblocks):
                x = xv[:, k * LANES:(k + 1) * LANES].astype(f32)
                sq = sq + x * x
            inv = lax.rsqrt(jnp.sum(sq, axis=1, keepdims=True) / dim + NORM_EPS)

            def normed(kb):
                x = xv[:, pl.ds(pl.multiple_of(kb * LANES, LANES), LANES)].astype(f32)
                return (x * inv * gf[pl.ds(kb, 1), :]).astype(jnp.bfloat16)

            for i in range(parts):
                nf[i] = normed(block_of(t, i)).astype(f32)
            with jax.named_scope('barr'):
                pl.semaphore_wait(barrier, 3)
            for i in range(parts):
                y_copy(i).start()
            id_copy.start()
            for k in range(kblocks):
                nb[:rows, k * LANES:(k + 1) * LANES] = normed(k)

            def forward_y(i):
                y_copy(i).wait_recv()
                if i < crossing:
                    x_copy(i, t).start()
                a_copy(i, t).start()

            def forward_x(i):
                x_copy(i, nbr_t).wait_recv()
                b_copy(i, nbr_t).start()

            def load_tile(name):
                kt = kt_of(name)
                i = int(name[1:])
                with jax.named_scope('wait_' + name):
                    if name[0] == 'a':
                        tile_recv(sib_t, i, asend, arecv)
                    if name[0] == 'b':
                        tile_recv(far_t, i, bsend, brecv)
                for h in range(2):
                    nb[LANES:LANES + rows, pl.ds(pl.multiple_of(kt * TILE + h * LANES, LANES), LANES)] = (
                        pf[2 * kt + h].astype(jnp.bfloat16))

            def tiles_dot(names, r):
                z = None
                for name in names:
                    kt = kt_of(name)
                    one = lax.dot_general(wv[kt, r, :], nb[:, pl.ds(pl.multiple_of(kt * TILE, TILE), TILE)], NT,
                                          preferred_element_type=f32)
                    z = one if z is None else z + one
                return z

            pad = jnp.full((1, LANES - drafts * batch), -8, jnp.int32)
            own_ids = jnp.concatenate([idv[k:k + 1, :] - t * cols for k in range(drafts)] + [pad], axis=1)
            own_want = jnp.broadcast_to(jnp.right_shift(own_ids, 3), (8, LANES))
            zero = jnp.zeros((8, LANES), f32)

            def own_forward(e):
                for chunk, blocks in enumerate(OWN_FORWARDS):
                    if blocks:
                        @pl.when(e == chunk)
                        def _():
                            with jax.named_scope('fy'):
                                for i in blocks:
                                    forward_y(i)

            with jax.named_scope('waite'):
                head_copy.wait()
            e_copy(1).start()
            with jax.named_scope('own'):
                z = lax.dot_general(hv[...], nb[:LANES, :], NT, preferred_element_type=f32)
                own_carry = update_stats(z, own_want, (None, None, None, zero))

            def own_step(e, carry):
                with jax.named_scope('waite'):
                    e_copy(e).wait()

                @pl.when(e + 2 < chunks)
                def _():
                    e_copy(e + 2).start()

                for chunk, groups in ((2, (0,)), (3, (1, 2))):
                    @pl.when(e == chunk)
                    def _():
                        for group in groups:
                            w_start(group)

                with jax.named_scope('own'):
                    z = lax.dot_general(ev[e], nb[:LANES, :], NT, preferred_element_type=f32)
                    carry = update_stats(z, own_want - (FIRST + e * CHUNK) // 8, carry)
                own_forward(e)
                return carry

            own_carry = lax.fori_loop(0, chunks, own_step, own_carry)
            own_carry = keep_row(own_carry, own_ids)

            for n_step, (ys, xs, names) in enumerate(STEPS[:-1]):
                for i in ys:
                    with jax.named_scope('fy'):
                        forward_y(i)
                for i in xs:
                    with jax.named_scope('fx'):
                        forward_x(i)
                for name in names:
                    load_tile(name)
                with jax.named_scope('ww'):
                    w_wait(n_step)
                if n_step + 3 < len(STEPS):
                    w_start(n_step + 3)

                @pl.when(t >= 0)
                def _():
                    with jax.named_scope('step'):
                        for n in range(nblocks):
                            r = slice(n * BLOCK, (n + 1) * BLOCK)
                            z = tiles_dot(names, r)
                            acc[r, :] = z if n_step == 0 else acc[r, :] + z

            id_copy.wait_recv()
            base = t * cols + OWN + y * half
            ids = jnp.concatenate([idv[k:k + 1, :] - base for k in range(drafts)] + [pad]
                                  + [idp[k:k + 1, :] - base for k in range(drafts)] + [pad], axis=1)
            want = jnp.broadcast_to(jnp.right_shift(ids, 3), (8, 2 * LANES))
            for name in STEPS[-1][2]:
                load_tile(name)
            with jax.named_scope('ww'):
                w_wait(len(STEPS) - 1)
            carry = (None, None, None, jnp.zeros((8, 2 * LANES), f32))
            with jax.named_scope('final'):
                for n in range(half // LAST):
                    r = slice(n * LAST, (n + 1) * LAST)
                    z = acc[r, :] + tiles_dot(STEPS[-1][2], r)
                    carry = update_stats(z, want - n * LAST // 8, carry)
            carry = keep_row(carry, ids)
            mine = pack_stats(merge_stats(own_carry, [c[:, :LANES] for c in carry]))
            theirs = pack_stats([c[:, LANES:] for c in carry])
            slot = y * tp + t
            for k in range(4):
                st[0, k:k + 1, :] = mine[k]
                st[1, k:k + 1, :] = theirs[k]
                rs[slot, k:k + 1, :] = mine[k]

            def s_copy(pd, pt, dy, k, into):
                return pltpu.make_async_remote_copy(
                    src_ref=st.at[dy], dst_ref=rs.at[into], send_sem=ssem, recv_sem=rsem,
                    device_id=(pd, pt), device_id_type=MESH)

            for pd, pt, dy, k in peers:
                s_copy(pd, pt, dy, k, slot).start()
            for sem, count in ((ysend, parts), (xsend, crossing), (asend, parts), (bsend, crossing)):
                sent = nf.at[pl.ds(0, count)]
                pltpu.make_async_remote_copy(
                    src_ref=sent, dst_ref=sent, send_sem=sem, recv_sem=irecv, device_id=sib, device_id_type=MESH).wait_send()
            id_copy.wait_send()
            with jax.named_scope('wstat'):
                every = rs.at[pl.ds(0, len(peers))]
                stats_copy = pltpu.make_async_remote_copy(
                    src_ref=every, dst_ref=every, send_sem=ssem, recv_sem=rsem, device_id=sib, device_id_type=MESH)
                stats_copy.wait_recv()
            with jax.named_scope('combine'):
                ms = [rs[k, 0:1, :] for k in range(2 * tp)]
                top = ms[0]
                for k in range(1, 2 * tp):
                    top = jnp.maximum(top, ms[k])
                s = jnp.zeros((1, LANES), f32)
                w = s
                p = s
                for k in range(2 * tp):
                    dm = ms[k] - top
                    f = jnp.exp(dm)
                    s = s + f * rs[k, 1:2, :]
                    w = w + f * (rs[k, 2:3, :] + dm * rs[k, 1:2, :])
                    p = p + rs[k, 3:4, :]
                log_sum = jnp.log(s)
                log_norm = top + log_sum
                ent = log_sum - w / s
                logp = p - log_norm
                for k in range(pos):
                    out[k:k + 1, :] = log_norm[:, k * batch:(k + 1) * batch]
                    out[pos + k:pos + k + 1, :] = ent[:, k * batch:(k + 1) * batch]
                    out[2 * pos + k:2 * pos + k + 1, :] = logp[:, k * batch:(k + 1) * batch]
            with jax.named_scope('wsend'):
                stats_copy.wait_send()

        hbm = pl.BlockSpec(memory_space=pl.ANY)
        vmem = pl.BlockSpec(memory_space=pltpu.VMEM)
        dma = pltpu.SemaphoreType.DMA
        bf16 = jnp.bfloat16
        packed = pl.pallas_call(
            kernel,
            out_shape=pltpu.VMEM((3 * pos, batch), f32),
            in_specs=[hbm] * 4,
            out_specs=vmem,
            scratch_shapes=[
                pltpu.VMEM((FIRST, dim), bf16),
                pltpu.VMEM((chunks, CHUNK, dim), bf16),
                pltpu.VMEM((tiles, half, TILE), bf16),
                pltpu.VMEM((rows, dim), bf16),
                pltpu.VMEM((2 * LANES, dim), bf16),
                pltpu.VMEM((parts, rows, LANES), f32),
                pltpu.VMEM((kblocks, rows, LANES), f32),
                pltpu.VMEM((half, 2 * LANES), f32),
                pltpu.VMEM((kblocks, LANES), bf16),
                pltpu.VMEM((kblocks, LANES), f32),
                pltpu.VMEM((drafts, batch), jnp.int32),
                pltpu.VMEM((drafts, batch), jnp.int32),
                pltpu.VMEM((2, 8, LANES), f32),
                pltpu.VMEM((2 * tp, 8, LANES), f32),
                dma((2,)),
                dma((len(STEPS),)),
                dma((4,)),
                dma, dma((parts,)),
                dma, dma((crossing,)),
                dma, dma((DIRECT,)),
                dma, dma((unique,)),
                dma, dma,
                dma, dma,
            ],
            compiler_params=pltpu.CompilerParams(
                collective_id=0, has_side_effects=True, vmem_limit_bytes=60 * 1024 * 1024),
        )(hidden.transpose(1, 0, 2).reshape(rows, dim), draft_ids.T, norm_gain.reshape(kblocks, LANES), head_w.T)

        def split(src, o_logp, o_logn, o_ent):
            o_logn[...] = src[:pos, :]
            o_ent[...] = src[pos:2 * pos, :]
            o_logp[...] = src[2 * pos:2 * pos + drafts, :]

        logp, logn, ent = pl.pallas_call(
            split,
            out_shape=[jax.ShapeDtypeStruct((drafts, batch), f32), jax.ShapeDtypeStruct((pos, batch), f32),
                       jax.ShapeDtypeStruct((pos, batch), f32)],
            in_specs=[vmem],
            out_specs=[vmem] * 3,
        )(pltpu.with_memory_space_constraint(packed, pltpu.VMEM))
        return logp.T, logn.T, ent.T

    specs_in = (P('dp', None, None), P('dp', None), P(None), P(None, 'tp'))
    specs_out = (P('dp', None), P('dp', None), P('dp', None))
    return jax.shard_map(per_device, mesh=mesh, in_specs=specs_in, out_specs=specs_out, check_vma=False)
```

```python
import jax
import jax.numpy as jnp
from jax import lax
from jax.experimental import pallas as pl
from jax.experimental.pallas import tpu as pltpu
from jax.sharding import PartitionSpec as P

NORM_EPS = 1e-5
MESH = pl.DeviceIdType.MESH
LANES = 128
TILE = 256
BLOCK = 800
OWN = 1600
FIRST = 160
CHUNK = 360
LAST = 320
DIRECT = 6
SHARED = 2
OWN_FORWARDS = ((), (0,), (1,), (2, 3))
STEPS = (
    ((), (), ('y0', 'y1', 'a0')),
    ((4, 5), (0,), ('a1', 'y2')),
    ((6,), (1,), ('x0', 'a2')),
    ((7,), (2, 3), ('y3', 'x1', 'b0')),
    ((8, 9), (4, 5), ('a3', 'b1', 'y4', 'x2')),
    ((10, 11), (6, 7), ('a4', 'b2', 'y5', 'x3')),
    ((), (), ('a5', 'b3')),
)
NT = (((1,), (1,)), ((), ()))


def update_stats(z, want, carry, first=None):
    z3 = z.reshape(-1, 8, z.shape[-1])
    bm = jnp.max(z3, axis=0)
    m, s, w, p = carry
    for g in range(z3.shape[0]):
        p = jnp.where(want == g, z3[g], p)
    if m is None:
        sh = z3 - bm[None]
        e = jnp.exp(sh)
        return bm, jnp.sum(e, axis=0), jnp.sum(e * sh, axis=0), p
    mn = jnp.maximum(m, bm)
    dm = m - mn
    a = jnp.exp(dm)
    sh = z3 - mn[None]
    e = jnp.exp(sh)
    w = a * (w + dm * s) + jnp.sum(e * sh, axis=0)
    s = a * s + jnp.sum(e, axis=0)
    return mn, s, w, p


def merge_stats(a, b):
    top = jnp.maximum(a[0], b[0])
    da, db = a[0] - top, b[0] - top
    fa, fb = jnp.exp(da), jnp.exp(db)
    return (
        top,
        fa * a[1] + fb * b[1],
        fa * (a[2] + da * a[1]) + fb * (b[2] + db * b[1]),
        a[3] + b[3],
    )


def keep_row(carry, ids):
    m, s, w, p = carry
    sub = lax.broadcasted_iota(jnp.int32, p.shape, 0)
    return m, s, w, jnp.where(sub == jnp.bitwise_and(ids, 7), p, 0.0)


def pack_stats(carry):
    m, s, w, p = carry
    top = jnp.max(m, axis=0, keepdims=True)
    dm = m - top
    f = jnp.exp(dm)
    return (
        top,
        jnp.sum(f * s, axis=0, keepdims=True),
        jnp.sum(f * (w + dm * s), axis=0, keepdims=True),
        jnp.sum(p, axis=0, keepdims=True),
    )


def solution(mesh):
    tp = mesh.shape['tp']

    def per_device(hidden, draft_ids, norm_gain, head_w):
        batch, pos, dim = hidden.shape
        drafts = draft_ids.shape[1]
        cols = head_w.shape[1]
        half = (cols - OWN) // 2
        chunks = (OWN - FIRST) // CHUNK
        rows = batch * pos
        kblocks = dim // LANES
        tiles = dim // TILE
        unique = DIRECT - SHARED
        assert tiles == tp * unique + 2 * SHARED
        parts = 2 * DIRECT
        crossing = 2 * unique
        nblocks = half // BLOCK
        f32 = jnp.float32

        def kernel(x_hbm, ids_hbm, g_hbm, w_hbm, out,
                   hv, ev, wv, xv, nb, nf, pf, acc, gv, gf, idv, idp, st, rs,
                   esem, wsem, lsem, ysend, yrecv, xsend, xrecv, asend, arecv, bsend, brecv, isend, irecv, ssem, rsem):
            t = lax.axis_index('tp')
            d = lax.axis_index('dp')
            y = lax.rem(d, 2)
            core = lax.rem(t, 2)
            mate = (d + 1 - 2 * y, t)
            sib = (d, t + 1 - 2 * core)
            nbr_t = lax.rem(t + 2, tp)
            nbr = (d, nbr_t)
            sib_t = t + 1 - 2 * core
            far_t = lax.rem(sib_t + 2, tp)

            cx = pltpu.make_async_copy(x_hbm, xv, lsem.at[0])
            cg = pltpu.make_async_copy(g_hbm, gv, lsem.at[1])
            ci = pltpu.make_async_copy(ids_hbm, idv, lsem.at[2])
            cg.start()
            ci.start()
            for k in range(pos):
                part = pl.ds(k * batch, batch)
                pltpu.make_async_copy(x_hbm.at[part], xv.at[part], lsem.at[0]).start()

            def w_copy(kt, group):
                return pltpu.make_async_copy(
                    w_hbm.at[pl.ds(pl.multiple_of(OWN + y * half, 16), half), pl.ds(pl.multiple_of(kt * TILE, TILE), TILE)],
                    wv.at[kt], wsem.at[group])

            def w_start(group):
                for name in STEPS[group][2]:
                    w_copy(kt_of(name), group).start()

            def w_wait(group):
                some = wv.at[pl.ds(0, len(STEPS[group][2]))]
                pltpu.make_async_copy(some, some, wsem.at[group]).wait()

            def tile_of(owner, i):
                if i < unique:
                    return owner * unique + i
                return tp * unique + lax.rem(owner, 2) * SHARED + i - unique

            def block_of(owner, i):
                return 2 * tile_of(owner, i // 2) + i % 2

            stream_t = {'y': t, 'a': sib_t, 'x': nbr_t, 'b': far_t}

            def kt_of(name):
                return tile_of(stream_t[name[0]], int(name[1:]))

            def e_copy(e):
                return pltpu.make_async_copy(
                    w_hbm.at[pl.ds(pl.multiple_of(FIRST + e * CHUNK, 8), CHUNK), :], ev.at[e], esem.at[lax.rem(e, 2)])

            head_copy = pltpu.make_async_copy(w_hbm.at[pl.ds(0, FIRST), :], hv, lsem.at[3])
            head_copy.start()
            e_copy(0).start()
            barrier = pltpu.get_barrier_semaphore()
            peers = []
            for dy in range(2):
                for k in range(tp):
                    if dy or k:
                        peers.append((mate[0] if dy else d, lax.rem(t + k, tp), dy, k))
            for near in (mate, sib, nbr):
                pl.semaphore_signal(barrier, inc=1, device_id=near, device_id_type=MESH)

            def y_copy(i):
                return pltpu.make_async_remote_copy(
                    src_ref=nf.at[i], dst_ref=pf.at[block_of(t, i)], send_sem=ysend, recv_sem=yrecv.at[i],
                    device_id=mate, device_id_type=MESH)

            def x_copy(i, owner):
                kb = block_of(owner, i)
                return pltpu.make_async_remote_copy(
                    src_ref=pf.at[kb], dst_ref=pf.at[kb], send_sem=xsend, recv_sem=xrecv.at[i],
                    device_id=nbr, device_id_type=MESH)

            def a_copy(i, owner):
                kb = block_of(owner, i)
                return pltpu.make_async_remote_copy(
                    src_ref=pf.at[kb], dst_ref=pf.at[kb], send_sem=asend, recv_sem=arecv.at[i // 2],
                    device_id=sib, device_id_type=MESH)

            def b_copy(i, owner):
                kb = block_of(owner, i)
                return pltpu.make_async_remote_copy(
                    src_ref=pf.at[kb], dst_ref=pf.at[kb], send_sem=bsend, recv_sem=brecv.at[i // 2],
                    device_id=sib, device_id_type=MESH)

            def tile_recv(owner, i, send, recv):
                both = pf.at[pl.ds(2 * tile_of(owner, i), 2)]
                pltpu.make_async_remote_copy(
                    src_ref=both, dst_ref=both, send_sem=send, recv_sem=recv.at[i],
                    device_id=sib, device_id_type=MESH).wait_recv()

            id_copy = pltpu.make_async_remote_copy(
                src_ref=idv, dst_ref=idp, send_sem=isend, recv_sem=irecv, device_id=mate, device_id_type=MESH)

            nb[rows:LANES, :] = jnp.zeros((LANES - rows, dim), jnp.bfloat16)
            nb[LANES + rows:, :] = jnp.zeros((LANES - rows, dim), jnp.bfloat16)
            with jax.named_scope('waitx'):
                cx.wait()
            sq = jnp.zeros((rows, LANES), f32)
            for k in range(kblocks):
                x = xv[:, k * LANES:(k + 1) * LANES].astype(f32)
                sq = sq + x * x
            inv = lax.rsqrt(jnp.sum(sq, axis=1, keepdims=True) / dim + NORM_EPS)

            with jax.named_scope('waitg'):
                ci.wait()
                cg.wait()
            gf[...] = gv[...].astype(f32)

            def normed(kb):
                x = xv[:, pl.ds(pl.multiple_of(kb * LANES, LANES), LANES)].astype(f32)
                return (x * inv * gf[pl.ds(kb, 1), :]).astype(jnp.bfloat16)

            for i in range(parts):
                nf[i] = normed(block_of(t, i)).astype(f32)
            e_copy(1).start()
            with jax.named_scope('barr'):
                pl.semaphore_wait(barrier, 3)
            for i in range(parts):
                y_copy(i).start()
            id_copy.start()
            for k in range(kblocks):
                nb[:rows, k * LANES:(k + 1) * LANES] = normed(k)

            def forward_y(i):
                y_copy(i).wait_recv()
                if i < crossing:
                    x_copy(i, t).start()
                a_copy(i, t).start()

            def forward_x(i):
                x_copy(i, nbr_t).wait_recv()
                b_copy(i, nbr_t).start()

            def load_tile(name):
                kt = kt_of(name)
                i = int(name[1:])
                with jax.named_scope('wait_' + name):
                    if name[0] == 'a':
                        tile_recv(sib_t, i, asend, arecv)
                    if name[0] == 'b':
                        tile_recv(far_t, i, bsend, brecv)
                for h in range(2):
                    nb[LANES:LANES + rows, pl.ds(pl.multiple_of(kt * TILE + h * LANES, LANES), LANES)] = (
                        pf[2 * kt + h].astype(jnp.bfloat16))

            def tiles_dot(names, r):
                z = None
                for name in names:
                    kt = kt_of(name)
                    one = lax.dot_general(wv[kt, r, :], nb[:, pl.ds(pl.multiple_of(kt * TILE, TILE), TILE)], NT,
                                          preferred_element_type=f32)
                    z = one if z is None else z + one
                return z

            pad = jnp.full((1, LANES - drafts * batch), -8, jnp.int32)
            own_ids = jnp.concatenate([idv[k:k + 1, :] - t * cols for k in range(drafts)] + [pad], axis=1)
            own_want = jnp.broadcast_to(jnp.right_shift(own_ids, 3), (8, LANES))
            zero = jnp.zeros((8, LANES), f32)

            def own_forward(e):
                for chunk, blocks in enumerate(OWN_FORWARDS):
                    if blocks:
                        @pl.when(e == chunk)
                        def _():
                            with jax.named_scope('fy'):
                                for i in blocks:
                                    forward_y(i)

            with jax.named_scope('waite'):
                head_copy.wait()
            with jax.named_scope('own'):
                z = lax.dot_general(hv[...], nb[:LANES, :], NT, preferred_element_type=f32)
                own_carry = update_stats(z, own_want, (None, None, None, zero))

            def own_step(e, carry):
                with jax.named_scope('waite'):
                    e_copy(e).wait()

                @pl.when(e + 2 < chunks)
                def _():
                    e_copy(e + 2).start()

                for chunk, groups in ((2, (0,)), (3, (1, 2))):
                    @pl.when(e == chunk)
                    def _():
                        for group in groups:
                            w_start(group)

                with jax.named_scope('own'):
                    z = lax.dot_general(ev[e], nb[:LANES, :], NT, preferred_element_type=f32)
                    carry = update_stats(z, own_want - (FIRST + e * CHUNK) // 8, carry)
                own_forward(e)
                return carry

            own_carry = lax.fori_loop(0, chunks, own_step, own_carry)
            own_carry = keep_row(own_carry, own_ids)

            for n_step, (ys, xs, names) in enumerate(STEPS[:-1]):
                for i in ys:
                    with jax.named_scope('fy'):
                        forward_y(i)
                for i in xs:
                    with jax.named_scope('fx'):
                        forward_x(i)
                for name in names:
                    load_tile(name)
                with jax.named_scope('ww'):
                    w_wait(n_step)
                if n_step + 3 < len(STEPS):
                    w_start(n_step + 3)

                @pl.when(t >= 0)
                def _():
                    with jax.named_scope('step'):
                        for n in range(nblocks):
                            r = slice(n * BLOCK, (n + 1) * BLOCK)
                            z = tiles_dot(names, r)
                            acc[r, :] = z if n_step == 0 else acc[r, :] + z

            id_copy.wait_recv()
            base = t * cols + OWN + y * half
            ids = jnp.concatenate([idv[k:k + 1, :] - base for k in range(drafts)] + [pad]
                                  + [idp[k:k + 1, :] - base for k in range(drafts)] + [pad], axis=1)
            want = jnp.broadcast_to(jnp.right_shift(ids, 3), (8, 2 * LANES))
            for name in STEPS[-1][2]:
                load_tile(name)
            with jax.named_scope('ww'):
                w_wait(len(STEPS) - 1)
            carry = (None, None, None, jnp.zeros((8, 2 * LANES), f32))
            with jax.named_scope('final'):
                for n in range(half // LAST):
                    r = slice(n * LAST, (n + 1) * LAST)
                    z = acc[r, :] + tiles_dot(STEPS[-1][2], r)
                    carry = update_stats(z, want - n * LAST // 8, carry)
            carry = keep_row(carry, ids)
            mine = pack_stats(merge_stats(own_carry, [c[:, :LANES] for c in carry]))
            theirs = pack_stats([c[:, LANES:] for c in carry])
            slot = y * tp + t
            for k in range(4):
                st[0, k:k + 1, :] = mine[k]
                st[1, k:k + 1, :] = theirs[k]
                rs[slot, k:k + 1, :] = mine[k]

            def s_copy(pd, pt, dy, k, into):
                return pltpu.make_async_remote_copy(
                    src_ref=st.at[dy], dst_ref=rs.at[into], send_sem=ssem, recv_sem=rsem,
                    device_id=(pd, pt), device_id_type=MESH)

            for pd, pt, dy, k in peers:
                s_copy(pd, pt, dy, k, slot).start()
            for sem, count in ((ysend, parts), (xsend, crossing), (asend, parts), (bsend, crossing)):
                sent = nf.at[pl.ds(0, count)]
                pltpu.make_async_remote_copy(
                    src_ref=sent, dst_ref=sent, send_sem=sem, recv_sem=irecv, device_id=sib, device_id_type=MESH).wait_send()
            id_copy.wait_send()
            with jax.named_scope('wstat'):
                every = rs.at[pl.ds(0, len(peers))]
                stats_copy = pltpu.make_async_remote_copy(
                    src_ref=every, dst_ref=every, send_sem=ssem, recv_sem=rsem, device_id=sib, device_id_type=MESH)
                stats_copy.wait_recv()
            with jax.named_scope('combine'):
                ms = [rs[k, 0:1, :] for k in range(2 * tp)]
                top = ms[0]
                for k in range(1, 2 * tp):
                    top = jnp.maximum(top, ms[k])
                s = jnp.zeros((1, LANES), f32)
                w = s
                p = s
                for k in range(2 * tp):
                    dm = ms[k] - top
                    f = jnp.exp(dm)
                    s = s + f * rs[k, 1:2, :]
                    w = w + f * (rs[k, 2:3, :] + dm * rs[k, 1:2, :])
                    p = p + rs[k, 3:4, :]
                log_sum = jnp.log(s)
                log_norm = top + log_sum
                ent = log_sum - w / s
                logp = p - log_norm
                for k in range(pos):
                    out[k:k + 1, :] = log_norm[:, k * batch:(k + 1) * batch]
                    out[pos + k:pos + k + 1, :] = ent[:, k * batch:(k + 1) * batch]
                    out[2 * pos + k:2 * pos + k + 1, :] = logp[:, k * batch:(k + 1) * batch]
            with jax.named_scope('wsend'):
                stats_copy.wait_send()

        hbm = pl.BlockSpec(memory_space=pl.ANY)
        vmem = pl.BlockSpec(memory_space=pltpu.VMEM)
        dma = pltpu.SemaphoreType.DMA
        bf16 = jnp.bfloat16
        packed = pl.pallas_call(
            kernel,
            out_shape=pltpu.VMEM((3 * pos, batch), f32),
            in_specs=[hbm] * 4,
            out_specs=vmem,
            scratch_shapes=[
                pltpu.VMEM((FIRST, dim), bf16),
                pltpu.VMEM((chunks, CHUNK, dim), bf16),
                pltpu.VMEM((tiles, half, TILE), bf16),
                pltpu.VMEM((rows, dim), bf16),
                pltpu.VMEM((2 * LANES, dim), bf16),
                pltpu.VMEM((parts, rows, LANES), f32),
                pltpu.VMEM((kblocks, rows, LANES), f32),
                pltpu.VMEM((half, 2 * LANES), f32),
                pltpu.VMEM((kblocks, LANES), bf16),
                pltpu.VMEM((kblocks, LANES), f32),
                pltpu.VMEM((drafts, batch), jnp.int32),
                pltpu.VMEM((drafts, batch), jnp.int32),
                pltpu.VMEM((2, 8, LANES), f32),
                pltpu.VMEM((2 * tp, 8, LANES), f32),
                dma((2,)),
                dma((len(STEPS),)),
                dma((4,)),
                dma, dma((parts,)),
                dma, dma((crossing,)),
                dma, dma((DIRECT,)),
                dma, dma((unique,)),
                dma, dma,
                dma, dma,
            ],
            compiler_params=pltpu.CompilerParams(
                collective_id=0, has_side_effects=True, vmem_limit_bytes=60 * 1024 * 1024),
        )(hidden.transpose(1, 0, 2).reshape(rows, dim), draft_ids.T, norm_gain.reshape(kblocks, LANES), head_w.T)

        def split(src, o_logp, o_logn, o_ent):
            o_logn[...] = src[:pos, :]
            o_ent[...] = src[pos:2 * pos, :]
            o_logp[...] = src[2 * pos:2 * pos + drafts, :]

        logp, logn, ent = pl.pallas_call(
            split,
            out_shape=[jax.ShapeDtypeStruct((drafts, batch), f32), jax.ShapeDtypeStruct((pos, batch), f32),
                       jax.ShapeDtypeStruct((pos, batch), f32)],
            in_specs=[vmem],
            out_specs=[vmem] * 3,
        )(pltpu.with_memory_space_constraint(packed, pltpu.VMEM))
        return logp.T, logn.T, ent.T

    specs_in = (P('dp', None, None), P('dp', None), P(None), P(None, 'tp'))
    specs_out = (P('dp', None), P('dp', None), P('dp', None))
    return jax.shard_map(per_device, mesh=mesh, in_specs=specs_in, out_specs=specs_out, check_vma=False)
```

```python
import jax
import jax.numpy as jnp
from jax import lax
from jax.experimental import pallas as pl
from jax.experimental.pallas import tpu as pltpu
from jax.sharding import PartitionSpec as P

NORM_EPS = 1e-5
MESH = pl.DeviceIdType.MESH
LANES = 128
TILE = 256
BLOCK = 800
OWN = 1600
FIRST = 160
CHUNK = 360
LAST = 320
DIRECT = 6
SHARED = 2
OWN_FORWARDS = ((), (0,), (1,), (2, 3))
STEPS = (
    ((), (), ('y0', 'y1', 'a0')),
    ((4, 5), (0,), ('a1', 'y2')),
    ((6,), (1,), ('x0', 'a2')),
    ((7,), (2, 3), ('y3', 'x1', 'b0')),
    ((8, 9), (4, 5), ('a3', 'b1', 'y4', 'x2')),
    ((10, 11), (6, 7), ('a4', 'b2', 'y5', 'x3')),
    ((), (), ('a5', 'b3')),
)
NT = (((1,), (1,)), ((), ()))


def update_stats(z, want, carry, first=None):
    z3 = z.reshape(-1, 8, z.shape[-1])
    bm = jnp.max(z3, axis=0)
    m, s, w, p = carry
    for g in range(z3.shape[0]):
        p = jnp.where(want == g, z3[g], p)
    if m is None:
        sh = z3 - bm[None]
        e = jnp.exp(sh)
        return bm, jnp.sum(e, axis=0), jnp.sum(e * sh, axis=0), p
    mn = jnp.maximum(m, bm)
    dm = m - mn
    a = jnp.exp(dm)
    sh = z3 - mn[None]
    e = jnp.exp(sh)
    w = a * (w + dm * s) + jnp.sum(e * sh, axis=0)
    s = a * s + jnp.sum(e, axis=0)
    return mn, s, w, p


def merge_stats(a, b):
    top = jnp.maximum(a[0], b[0])
    da, db = a[0] - top, b[0] - top
    fa, fb = jnp.exp(da), jnp.exp(db)
    return (
        top,
        fa * a[1] + fb * b[1],
        fa * (a[2] + da * a[1]) + fb * (b[2] + db * b[1]),
        a[3] + b[3],
    )


def keep_row(carry, ids):
    m, s, w, p = carry
    sub = lax.broadcasted_iota(jnp.int32, p.shape, 0)
    return m, s, w, jnp.where(sub == jnp.bitwise_and(ids, 7), p, 0.0)


def pack_stats(carry):
    m, s, w, p = carry
    top = jnp.max(m, axis=0, keepdims=True)
    dm = m - top
    f = jnp.exp(dm)
    return (
        top,
        jnp.sum(f * s, axis=0, keepdims=True),
        jnp.sum(f * (w + dm * s), axis=0, keepdims=True),
        jnp.sum(p, axis=0, keepdims=True),
    )


def solution(mesh):
    tp = mesh.shape['tp']

    def per_device(hidden, draft_ids, norm_gain, head_w):
        batch, pos, dim = hidden.shape
        drafts = draft_ids.shape[1]
        cols = head_w.shape[1]
        half = (cols - OWN) // 2
        chunks = (OWN - FIRST) // CHUNK
        rows = batch * pos
        kblocks = dim // LANES
        tiles = dim // TILE
        unique = DIRECT - SHARED
        assert tiles == tp * unique + 2 * SHARED
        parts = 2 * DIRECT
        crossing = 2 * unique
        nblocks = half // BLOCK
        f32 = jnp.float32

        def kernel(x_hbm, ids_hbm, g_hbm, w_hbm, out,
                   hv, ev, wv, xv, nb, nf, pf, acc, gv, gf, idv, idp, st, rs,
                   esem, wsem, lsem, ysend, yrecv, xsend, xrecv, asend, arecv, bsend, brecv, isend, irecv, ssem, rsem):
            t = lax.axis_index('tp')
            d = lax.axis_index('dp')
            y = lax.rem(d, 2)
            core = lax.rem(t, 2)
            mate = (d + 1 - 2 * y, t)
            sib = (d, t + 1 - 2 * core)
            nbr_t = lax.rem(t + 2, tp)
            nbr = (d, nbr_t)
            sib_t = t + 1 - 2 * core
            far_t = lax.rem(sib_t + 2, tp)

            cx = pltpu.make_async_copy(x_hbm, xv, lsem.at[0])
            cg = pltpu.make_async_copy(g_hbm, gv, lsem.at[1])
            ci = pltpu.make_async_copy(ids_hbm, idv, lsem.at[2])
            cg.start()
            ci.start()
            for k in range(pos):
                part = pl.ds(k * batch, batch)
                pltpu.make_async_copy(x_hbm.at[part], xv.at[part], lsem.at[0]).start()

            def w_copy(kt, group):
                return pltpu.make_async_copy(
                    w_hbm.at[pl.ds(pl.multiple_of(OWN + y * half, 16), half), pl.ds(pl.multiple_of(kt * TILE, TILE), TILE)],
                    wv.at[kt], wsem.at[group])

            def w_start(group):
                for name in STEPS[group][2]:
                    w_copy(kt_of(name), group).start()

            def w_wait(group):
                some = wv.at[pl.ds(0, len(STEPS[group][2]))]
                pltpu.make_async_copy(some, some, wsem.at[group]).wait()

            def tile_of(owner, i):
                if i < unique:
                    return owner * unique + i
                return tp * unique + lax.rem(owner, 2) * SHARED + i - unique

            def block_of(owner, i):
                return 2 * tile_of(owner, i // 2) + i % 2

            stream_t = {'y': t, 'a': sib_t, 'x': nbr_t, 'b': far_t}

            def kt_of(name):
                return tile_of(stream_t[name[0]], int(name[1:]))

            def e_copy(e):
                return pltpu.make_async_copy(
                    w_hbm.at[pl.ds(pl.multiple_of(FIRST + e * CHUNK, 8), CHUNK), :], ev.at[e], esem.at[lax.rem(e, 2)])

            head_copy = pltpu.make_async_copy(w_hbm.at[pl.ds(0, FIRST), :], hv, lsem.at[3])
            head_copy.start()
            e_copy(0).start()
            barrier = pltpu.get_barrier_semaphore()
            peers = []
            for dy in range(2):
                for k in range(tp):
                    if dy or k:
                        peers.append((mate[0] if dy else d, lax.rem(t + k, tp), dy, k))
            for near in (mate, sib, nbr):
                pl.semaphore_signal(barrier, inc=1, device_id=near, device_id_type=MESH)

            def y_copy(i):
                return pltpu.make_async_remote_copy(
                    src_ref=nf.at[i], dst_ref=pf.at[block_of(t, i)], send_sem=ysend, recv_sem=yrecv.at[i],
                    device_id=mate, device_id_type=MESH)

            def x_copy(i, owner):
                kb = block_of(owner, i)
                return pltpu.make_async_remote_copy(
                    src_ref=pf.at[kb], dst_ref=pf.at[kb], send_sem=xsend, recv_sem=xrecv.at[i],
                    device_id=nbr, device_id_type=MESH)

            def a_copy(i, owner):
                kb = block_of(owner, i)
                return pltpu.make_async_remote_copy(
                    src_ref=pf.at[kb], dst_ref=pf.at[kb], send_sem=asend, recv_sem=arecv.at[i // 2],
                    device_id=sib, device_id_type=MESH)

            def b_copy(i, owner):
                kb = block_of(owner, i)
                return pltpu.make_async_remote_copy(
                    src_ref=pf.at[kb], dst_ref=pf.at[kb], send_sem=bsend, recv_sem=brecv.at[i // 2],
                    device_id=sib, device_id_type=MESH)

            def tile_recv(owner, i, send, recv):
                both = pf.at[pl.ds(2 * tile_of(owner, i), 2)]
                pltpu.make_async_remote_copy(
                    src_ref=both, dst_ref=both, send_sem=send, recv_sem=recv.at[i],
                    device_id=sib, device_id_type=MESH).wait_recv()

            id_copy = pltpu.make_async_remote_copy(
                src_ref=idv, dst_ref=idp, send_sem=isend, recv_sem=irecv, device_id=mate, device_id_type=MESH)

            nb[rows:LANES, :] = jnp.zeros((LANES - rows, dim), jnp.bfloat16)
            nb[LANES + rows:, :] = jnp.zeros((LANES - rows, dim), jnp.bfloat16)
            with jax.named_scope('waitx'):
                cx.wait()
            sq = jnp.zeros((rows, LANES), f32)
            for k in range(kblocks):
                x = xv[:, k * LANES:(k + 1) * LANES].astype(f32)
                sq = sq + x * x
            inv = lax.rsqrt(jnp.sum(sq, axis=1, keepdims=True) / dim + NORM_EPS)

            with jax.named_scope('waitg'):
                ci.wait()
                cg.wait()
            gf[...] = gv[...].astype(f32)

            def normed(kb):
                x = xv[:, pl.ds(pl.multiple_of(kb * LANES, LANES), LANES)].astype(f32)
                return (x * inv * gf[pl.ds(kb, 1), :]).astype(jnp.bfloat16)

            for i in range(parts):
                nf[i] = normed(block_of(t, i)).astype(f32)
            e_copy(1).start()
            with jax.named_scope('barr'):
                pl.semaphore_wait(barrier, 3)
            for i in range(parts):
                y_copy(i).start()
            id_copy.start()
            for k in range(kblocks):
                nb[:rows, k * LANES:(k + 1) * LANES] = normed(k)

            def forward_y(i):
                y_copy(i).wait_recv()
                if i < crossing:
                    x_copy(i, t).start()
                a_copy(i, t).start()

            def forward_x(i):
                x_copy(i, nbr_t).wait_recv()
                b_copy(i, nbr_t).start()

            def load_tile(name):
                kt = kt_of(name)
                i = int(name[1:])
                with jax.named_scope('wait_' + name):
                    if name[0] == 'a':
                        tile_recv(sib_t, i, asend, arecv)
                    if name[0] == 'b':
                        tile_recv(far_t, i, bsend, brecv)
                for h in range(2):
                    nb[LANES:LANES + rows, pl.ds(pl.multiple_of(kt * TILE + h * LANES, LANES), LANES)] = (
                        pf[2 * kt + h].astype(jnp.bfloat16))

            def tiles_dot(names, r):
                z = None
                for name in names:
                    kt = kt_of(name)
                    one = lax.dot_general(wv[kt, r, :], nb[:, pl.ds(pl.multiple_of(kt * TILE, TILE), TILE)], NT,
                                          preferred_element_type=f32)
                    z = one if z is None else z + one
                return z

            pad = jnp.full((1, LANES - drafts * batch), -8, jnp.int32)
            own_ids = jnp.concatenate([idv[k:k + 1, :] - t * cols for k in range(drafts)] + [pad], axis=1)
            own_want = jnp.broadcast_to(jnp.right_shift(own_ids, 3), (8, LANES))
            zero = jnp.zeros((8, LANES), f32)

            def own_forward(e):
                for chunk, blocks in enumerate(OWN_FORWARDS):
                    if blocks:
                        @pl.when(e == chunk)
                        def _():
                            with jax.named_scope('fy'):
                                for i in blocks:
                                    forward_y(i)

            with jax.named_scope('waite'):
                head_copy.wait()
            with jax.named_scope('own'):
                z = lax.dot_general(hv[...], nb[:LANES, :], NT, preferred_element_type=f32)
                own_carry = update_stats(z, own_want, (None, None, None, zero))

            def own_step(e, carry):
                with jax.named_scope('waite'):
                    e_copy(e).wait()

                @pl.when(e + 2 < chunks)
                def _():
                    e_copy(e + 2).start()

                for chunk, groups in ((2, (0,)), (3, (1, 2))):
                    @pl.when(e == chunk)
                    def _():
                        for group in groups:
                            w_start(group)

                with jax.named_scope('own'):
                    pl.delay(1)
                    z = lax.dot_general(ev[e], nb[:LANES, :], NT, preferred_element_type=f32)
                    carry = update_stats(z, own_want - (FIRST + e * CHUNK) // 8, carry)
                own_forward(e)
                return carry

            own_carry = lax.fori_loop(0, chunks, own_step, own_carry)
            own_carry = keep_row(own_carry, own_ids)

            for n_step, (ys, xs, names) in enumerate(STEPS[:-1]):
                for i in ys:
                    with jax.named_scope('fy'):
                        forward_y(i)
                for i in xs:
                    with jax.named_scope('fx'):
                        forward_x(i)
                for name in names:
                    load_tile(name)
                with jax.named_scope('ww'):
                    w_wait(n_step)
                if n_step + 3 < len(STEPS):
                    w_start(n_step + 3)

                @pl.when(t >= 0)
                def _():
                    with jax.named_scope('step'):
                        for n in range(nblocks):
                            r = slice(n * BLOCK, (n + 1) * BLOCK)
                            z = tiles_dot(names, r)
                            acc[r, :] = z if n_step == 0 else acc[r, :] + z

            id_copy.wait_recv()
            base = t * cols + OWN + y * half
            ids = jnp.concatenate([idv[k:k + 1, :] - base for k in range(drafts)] + [pad]
                                  + [idp[k:k + 1, :] - base for k in range(drafts)] + [pad], axis=1)
            want = jnp.broadcast_to(jnp.right_shift(ids, 3), (8, 2 * LANES))
            for name in STEPS[-1][2]:
                load_tile(name)
            with jax.named_scope('ww'):
                w_wait(len(STEPS) - 1)
            carry = (None, None, None, jnp.zeros((8, 2 * LANES), f32))
            with jax.named_scope('final'):
                for n in range(half // LAST):
                    r = slice(n * LAST, (n + 1) * LAST)
                    z = acc[r, :] + tiles_dot(STEPS[-1][2], r)
                    carry = update_stats(z, want - n * LAST // 8, carry)
            carry = keep_row(carry, ids)
            mine = pack_stats(merge_stats(own_carry, [c[:, :LANES] for c in carry]))
            theirs = pack_stats([c[:, LANES:] for c in carry])
            slot = y * tp + t
            for k in range(4):
                st[0, k:k + 1, :] = mine[k]
                st[1, k:k + 1, :] = theirs[k]
                rs[slot, k:k + 1, :] = mine[k]

            def s_copy(pd, pt, dy, k, into):
                return pltpu.make_async_remote_copy(
                    src_ref=st.at[dy], dst_ref=rs.at[into], send_sem=ssem, recv_sem=rsem,
                    device_id=(pd, pt), device_id_type=MESH)

            for pd, pt, dy, k in peers:
                s_copy(pd, pt, dy, k, slot).start()
            for sem, count in ((ysend, parts), (xsend, crossing), (asend, parts), (bsend, crossing)):
                sent = nf.at[pl.ds(0, count)]
                pltpu.make_async_remote_copy(
                    src_ref=sent, dst_ref=sent, send_sem=sem, recv_sem=irecv, device_id=sib, device_id_type=MESH).wait_send()
            id_copy.wait_send()
            with jax.named_scope('wstat'):
                every = rs.at[pl.ds(0, len(peers))]
                stats_copy = pltpu.make_async_remote_copy(
                    src_ref=every, dst_ref=every, send_sem=ssem, recv_sem=rsem, device_id=sib, device_id_type=MESH)
                stats_copy.wait_recv()
            with jax.named_scope('combine'):
                ms = [rs[k, 0:1, :] for k in range(2 * tp)]
                top = ms[0]
                for k in range(1, 2 * tp):
                    top = jnp.maximum(top, ms[k])
                s = jnp.zeros((1, LANES), f32)
                w = s
                p = s
                for k in range(2 * tp):
                    dm = ms[k] - top
                    f = jnp.exp(dm)
                    s = s + f * rs[k, 1:2, :]
                    w = w + f * (rs[k, 2:3, :] + dm * rs[k, 1:2, :])
                    p = p + rs[k, 3:4, :]
                log_sum = jnp.log(s)
                log_norm = top + log_sum
                ent = log_sum - w / s
                logp = p - log_norm
                for k in range(pos):
                    out[k:k + 1, :] = log_norm[:, k * batch:(k + 1) * batch]
                    out[pos + k:pos + k + 1, :] = ent[:, k * batch:(k + 1) * batch]
                    out[2 * pos + k:2 * pos + k + 1, :] = logp[:, k * batch:(k + 1) * batch]
            with jax.named_scope('wsend'):
                stats_copy.wait_send()

        hbm = pl.BlockSpec(memory_space=pl.ANY)
        vmem = pl.BlockSpec(memory_space=pltpu.VMEM)
        dma = pltpu.SemaphoreType.DMA
        bf16 = jnp.bfloat16
        packed = pl.pallas_call(
            kernel,
            out_shape=pltpu.VMEM((3 * pos, batch), f32),
            in_specs=[hbm] * 4,
            out_specs=vmem,
            scratch_shapes=[
                pltpu.VMEM((FIRST, dim), bf16),
                pltpu.VMEM((chunks, CHUNK, dim), bf16),
                pltpu.VMEM((tiles, half, TILE), bf16),
                pltpu.VMEM((rows, dim), bf16),
                pltpu.VMEM((2 * LANES, dim), bf16),
                pltpu.VMEM((parts, rows, LANES), f32),
                pltpu.VMEM((kblocks, rows, LANES), f32),
                pltpu.VMEM((half, 2 * LANES), f32),
                pltpu.VMEM((kblocks, LANES), bf16),
                pltpu.VMEM((kblocks, LANES), f32),
                pltpu.VMEM((drafts, batch), jnp.int32),
                pltpu.VMEM((drafts, batch), jnp.int32),
                pltpu.VMEM((2, 8, LANES), f32),
                pltpu.VMEM((2 * tp, 8, LANES), f32),
                dma((2,)),
                dma((len(STEPS),)),
                dma((4,)),
                dma, dma((parts,)),
                dma, dma((crossing,)),
                dma, dma((DIRECT,)),
                dma, dma((unique,)),
                dma, dma,
                dma, dma,
            ],
            compiler_params=pltpu.CompilerParams(
                collective_id=0, has_side_effects=True, vmem_limit_bytes=60 * 1024 * 1024),
        )(hidden.transpose(1, 0, 2).reshape(rows, dim), draft_ids.T, norm_gain.reshape(kblocks, LANES), head_w.T)

        def split(src, o_logp, o_logn, o_ent):
            o_logn[...] = src[:pos, :]
            o_ent[...] = src[pos:2 * pos, :]
            o_logp[...] = src[2 * pos:2 * pos + drafts, :]

        logp, logn, ent = pl.pallas_call(
            split,
            out_shape=[jax.ShapeDtypeStruct((drafts, batch), f32), jax.ShapeDtypeStruct((pos, batch), f32),
                       jax.ShapeDtypeStruct((pos, batch), f32)],
            in_specs=[vmem],
            out_specs=[vmem] * 3,
        )(pltpu.with_memory_space_constraint(packed, pltpu.VMEM))
        return logp.T, logn.T, ent.T

    specs_in = (P('dp', None, None), P('dp', None), P(None), P(None, 'tp'))
    specs_out = (P('dp', None), P('dp', None), P('dp', None))
    return jax.shard_map(per_device, mesh=mesh, in_specs=specs_in, out_specs=specs_out, check_vma=False)
```

```python
import jax
import jax.numpy as jnp
from jax import lax
from jax.experimental import pallas as pl
from jax.experimental.pallas import tpu as pltpu
from jax.sharding import PartitionSpec as P

NORM_EPS = 1e-5
MESH = pl.DeviceIdType.MESH
LANES = 128
TILE = 256
BLOCK = 800
OWN = 1600
FIRST = 400
CHUNK = 400
LAST = 320
DIRECT = 6
SHARED = 2
OWN_FORWARDS = ((0,), (1, 2), (3,))
STEPS = (
    ((), (), ('y0', 'a0', 'y1')),
    ((4, 5), (0, 1), ('a1', 'y2', 'x0')),
    ((6, 7), (2, 3), ('a2', 'b0', 'y3', 'x1')),
    ((8, 9), (4, 5), ('a3', 'b1', 'y4', 'x2')),
    ((10, 11), (6, 7), ('a4', 'b2')),
    ((), (), ('y5', 'x3', 'a5', 'b3')),
)
Y_GROUPS = tuple(g for g in OWN_FORWARDS + tuple(ys for ys, _, _ in STEPS) if g)
X_GROUPS = tuple(xs for _, xs, _ in STEPS if xs)


def group_of(groups, i):
    return [i in g for g in groups].index(True)


def step_of(kind, i):
    return [kind + str(i) in names for _, _, names in STEPS].index(True)


NT = (((1,), (1,)), ((), ()))


def update_stats(z, want, carry, first=None):
    z3 = z.reshape(-1, 8, z.shape[-1])
    bm = jnp.max(z3, axis=0)
    m, s, w, p = carry
    for g in range(z3.shape[0]):
        p = jnp.where(want == g, z3[g], p)
    if m is None:
        sh = z3 - bm[None]
        e = jnp.exp(sh)
        return bm, jnp.sum(e, axis=0), jnp.sum(e * sh, axis=0), p
    mn = jnp.maximum(m, bm)
    dm = m - mn
    a = jnp.exp(dm)
    sh = z3 - mn[None]
    e = jnp.exp(sh)
    w = a * (w + dm * s) + jnp.sum(e * sh, axis=0)
    s = a * s + jnp.sum(e, axis=0)
    return mn, s, w, p


def merge_stats(a, b):
    top = jnp.maximum(a[0], b[0])
    da, db = a[0] - top, b[0] - top
    fa, fb = jnp.exp(da), jnp.exp(db)
    return (
        top,
        fa * a[1] + fb * b[1],
        fa * (a[2] + da * a[1]) + fb * (b[2] + db * b[1]),
        a[3] + b[3],
    )


def keep_row(carry, ids):
    m, s, w, p = carry
    sub = lax.broadcasted_iota(jnp.int32, p.shape, 0)
    return m, s, w, jnp.where(sub == jnp.bitwise_and(ids, 7), p, 0.0)


def pack_stats(carry):
    m, s, w, p = carry
    top = jnp.max(m, axis=0, keepdims=True)
    dm = m - top
    f = jnp.exp(dm)
    return (
        top,
        jnp.sum(f * s, axis=0, keepdims=True),
        jnp.sum(f * (w + dm * s), axis=0, keepdims=True),
        jnp.sum(p, axis=0, keepdims=True),
    )


def solution(mesh):
    tp = mesh.shape['tp']

    def per_device(hidden, draft_ids, norm_gain, head_w):
        batch, pos, dim = hidden.shape
        drafts = draft_ids.shape[1]
        cols = head_w.shape[1]
        half = (cols - OWN) // 2
        chunks = (OWN - FIRST) // CHUNK
        rows = batch * pos
        kblocks = dim // LANES
        tiles = dim // TILE
        unique = DIRECT - SHARED
        assert tiles == tp * unique + 2 * SHARED
        parts = 2 * DIRECT
        crossing = 2 * unique
        assert 2 * (parts + crossing) == kblocks
        nblocks = half // BLOCK
        f32 = jnp.float32

        def kernel(x_hbm, ids_hbm, g_hbm, w_hbm, out,
                   hv, ev, wv, xv, nb, nf, pf, acc, gv, gf, idv, idp, st, rs,
                   esem, wsem, lsem, psend, yrecv, xrecv, srecv, isend, irecv, ssem, rsem):
            t = lax.axis_index('tp')
            d = lax.axis_index('dp')
            y = lax.rem(d, 2)
            core = lax.rem(t, 2)
            mate = (d + 1 - 2 * y, t)
            sib = (d, t + 1 - 2 * core)
            nbr_t = lax.rem(t + 2, tp)
            nbr = (d, nbr_t)
            sib_t = t + 1 - 2 * core
            far_t = lax.rem(sib_t + 2, tp)

            cx = pltpu.make_async_copy(x_hbm, xv, lsem.at[0])
            cg = pltpu.make_async_copy(g_hbm, gv, lsem.at[1])
            ci = pltpu.make_async_copy(ids_hbm, idv, lsem.at[2])
            cg.start()
            ci.start()
            for k in range(pos):
                part = pl.ds(k * batch, batch)
                pltpu.make_async_copy(x_hbm.at[part], xv.at[part], lsem.at[0]).start()

            def w_copy(kt, group):
                return pltpu.make_async_copy(
                    w_hbm.at[pl.ds(pl.multiple_of(OWN + y * half, 16), half), pl.ds(pl.multiple_of(kt * TILE, TILE), TILE)],
                    wv.at[kt], wsem.at[group])

            def w_start(group):
                for name in STEPS[group][2]:
                    w_copy(kt_of(name), group).start()

            def w_wait(group):
                some = wv.at[pl.ds(0, len(STEPS[group][2]))]
                pltpu.make_async_copy(some, some, wsem.at[group]).wait()

            def tile_of(owner, i):
                if i < unique:
                    return owner * unique + i
                return tp * unique + lax.rem(owner, 2) * SHARED + i - unique

            def block_of(owner, i):
                return 2 * tile_of(owner, i // 2) + i % 2

            stream_t = {'y': t, 'a': sib_t, 'x': nbr_t, 'b': far_t}

            def kt_of(name):
                return tile_of(stream_t[name[0]], int(name[1:]))

            def e_copy(e):
                return pltpu.make_async_copy(
                    w_hbm.at[pl.ds(pl.multiple_of(FIRST + e * CHUNK, 8), CHUNK), :], ev.at[e], esem.at[lax.rem(e, 2)])

            head_copy = pltpu.make_async_copy(w_hbm.at[pl.ds(0, FIRST), :], hv, lsem.at[3])
            head_copy.start()
            e_copy(0).start()
            barrier = pltpu.get_barrier_semaphore()
            peers = []
            for dy in range(2):
                for k in range(tp):
                    if dy or k:
                        peers.append((mate[0] if dy else d, lax.rem(t + k, tp), dy, k))
            for near in (mate, sib, nbr):
                pl.semaphore_signal(barrier, inc=1, device_id=near, device_id_type=MESH)

            def y_copy(i):
                return pltpu.make_async_remote_copy(
                    src_ref=nf.at[i], dst_ref=pf.at[block_of(t, i)], send_sem=psend, recv_sem=yrecv.at[group_of(Y_GROUPS, i)],
                    device_id=mate, device_id_type=MESH)

            def x_copy(i, owner):
                kb = block_of(owner, i)
                return pltpu.make_async_remote_copy(
                    src_ref=pf.at[kb], dst_ref=pf.at[kb], send_sem=psend, recv_sem=xrecv.at[group_of(X_GROUPS, i)],
                    device_id=nbr, device_id_type=MESH)

            def a_copy(i, owner):
                kb = block_of(owner, i)
                return pltpu.make_async_remote_copy(
                    src_ref=pf.at[kb], dst_ref=pf.at[kb], send_sem=psend, recv_sem=srecv.at[step_of('a', i // 2)],
                    device_id=sib, device_id_type=MESH)

            def b_copy(i, owner):
                kb = block_of(owner, i)
                return pltpu.make_async_remote_copy(
                    src_ref=pf.at[kb], dst_ref=pf.at[kb], send_sem=psend, recv_sem=srecv.at[step_of('b', i // 2)],
                    device_id=sib, device_id_type=MESH)

            def blocks_recv(count, recv):
                some = pf.at[pl.ds(0, count)]
                pltpu.make_async_remote_copy(
                    src_ref=some, dst_ref=some, send_sem=psend, recv_sem=recv,
                    device_id=sib, device_id_type=MESH).wait_recv()

            id_copy = pltpu.make_async_remote_copy(
                src_ref=idv, dst_ref=idp, send_sem=isend, recv_sem=irecv, device_id=mate, device_id_type=MESH)

            nb[rows:LANES, :] = jnp.zeros((LANES - rows, dim), jnp.bfloat16)
            nb[LANES + rows:, :] = jnp.zeros((LANES - rows, dim), jnp.bfloat16)
            with jax.named_scope('waitx'):
                cx.wait()
            sq = jnp.zeros((rows, LANES), f32)
            for k in range(kblocks):
                x = xv[:, k * LANES:(k + 1) * LANES].astype(f32)
                sq = sq + x * x
            inv = lax.rsqrt(jnp.sum(sq, axis=1, keepdims=True) / dim + NORM_EPS)

            with jax.named_scope('waitg'):
                ci.wait()
                cg.wait()
            gf[...] = gv[...].astype(f32)

            def normed(kb):
                x = xv[:, pl.ds(pl.multiple_of(kb * LANES, LANES), LANES)].astype(f32)
                return (x * inv * gf[pl.ds(kb, 1), :]).astype(jnp.bfloat16)

            for i in range(parts):
                nf[i] = normed(block_of(t, i)).astype(f32)
            e_copy(1).start()
            with jax.named_scope('barr'):
                pl.semaphore_wait(barrier, 3)
            for i in range(parts):
                y_copy(i).start()
            id_copy.start()
            for k in range(kblocks):
                nb[:rows, k * LANES:(k + 1) * LANES] = normed(k)

            def forward_y(group):
                if group:
                    blocks_recv(len(group), yrecv.at[group_of(Y_GROUPS, group[0])])
                for i in group:
                    if i < crossing:
                        x_copy(i, t).start()
                    a_copy(i, t).start()

            def forward_x(group):
                if group:
                    blocks_recv(len(group), xrecv.at[group_of(X_GROUPS, group[0])])
                for i in group:
                    b_copy(i, nbr_t).start()

            def sibling_wait(step):
                count = len([name for name in STEPS[step][2] if name[0] in 'ab'])
                if count:
                    blocks_recv(2 * count, srecv.at[step])

            def load_tile(name):
                kt = kt_of(name)
                for h in range(2):
                    nb[LANES:LANES + rows, pl.ds(pl.multiple_of(kt * TILE + h * LANES, LANES), LANES)] = (
                        pf[2 * kt + h].astype(jnp.bfloat16))

            def tiles_dot(names, r):
                z = None
                for name in names:
                    kt = kt_of(name)
                    one = lax.dot_general(wv[kt, r, :], nb[:, pl.ds(pl.multiple_of(kt * TILE, TILE), TILE)], NT,
                                          preferred_element_type=f32)
                    z = one if z is None else z + one
                return z

            pad = jnp.full((1, LANES - drafts * batch), -8, jnp.int32)
            own_ids = jnp.concatenate([idv[k:k + 1, :] - t * cols for k in range(drafts)] + [pad], axis=1)
            own_want = jnp.broadcast_to(jnp.right_shift(own_ids, 3), (8, LANES))
            zero = jnp.zeros((8, LANES), f32)

            def own_forward(e):
                for chunk, blocks in enumerate(OWN_FORWARDS):
                    if blocks:
                        @pl.when(e == chunk)
                        def _():
                            with jax.named_scope('fy'):
                                forward_y(blocks)

            with jax.named_scope('waite'):
                head_copy.wait()
            with jax.named_scope('own'):
                z = lax.dot_general(hv[...], nb[:LANES, :], NT, preferred_element_type=f32)
                own_carry = update_stats(z, own_want, (None, None, None, zero))

            def own_step(e, carry):
                with jax.named_scope('waite'):
                    e_copy(e).wait()

                @pl.when(e + 2 < chunks)
                def _():
                    e_copy(e + 2).start()

                for chunk, groups in ((1, (0,)), (2, (1, 2))):
                    @pl.when(e == chunk)
                    def _():
                        for group in groups:
                            w_start(group)

                with jax.named_scope('own'):
                    pl.delay(1)
                    z = lax.dot_general(ev[e], nb[:LANES, :], NT, preferred_element_type=f32)
                    carry = update_stats(z, own_want - (FIRST + e * CHUNK) // 8, carry)
                own_forward(e)
                return carry

            own_carry = lax.fori_loop(0, chunks, own_step, own_carry)
            own_carry = keep_row(own_carry, own_ids)

            for n_step, (ys, xs, names) in enumerate(STEPS[:-1]):
                with jax.named_scope('fy'):
                    forward_y(ys)
                with jax.named_scope('fx'):
                    forward_x(xs)
                with jax.named_scope('ws'):
                    sibling_wait(n_step)
                for name in names:
                    load_tile(name)
                with jax.named_scope('ww'):
                    w_wait(n_step)
                if n_step + 3 < len(STEPS):
                    w_start(n_step + 3)

                @pl.when(t >= 0)
                def _():
                    with jax.named_scope('step'):
                        for n in range(nblocks):
                            r = slice(n * BLOCK, (n + 1) * BLOCK)
                            z = tiles_dot(names, r)
                            acc[r, :] = z if n_step == 0 else acc[r, :] + z

            id_copy.wait_recv()
            base = t * cols + OWN + y * half
            ids = jnp.concatenate([idv[k:k + 1, :] - base for k in range(drafts)] + [pad]
                                  + [idp[k:k + 1, :] - base for k in range(drafts)] + [pad], axis=1)
            want = jnp.broadcast_to(jnp.right_shift(ids, 3), (8, 2 * LANES))
            sibling_wait(len(STEPS) - 1)
            for name in STEPS[-1][2]:
                load_tile(name)
            with jax.named_scope('ww'):
                w_wait(len(STEPS) - 1)
            carry = (None, None, None, jnp.zeros((8, 2 * LANES), f32))
            with jax.named_scope('final'):
                for n in range(half // LAST):
                    r = slice(n * LAST, (n + 1) * LAST)
                    z = acc[r, :] + tiles_dot(STEPS[-1][2], r)
                    carry = update_stats(z, want - n * LAST // 8, carry)
            carry = keep_row(carry, ids)
            mine = pack_stats(merge_stats(own_carry, [c[:, :LANES] for c in carry]))
            theirs = pack_stats([c[:, LANES:] for c in carry])
            slot = y * tp + t
            for k in range(4):
                st[0, k:k + 1, :] = mine[k]
                st[1, k:k + 1, :] = theirs[k]
                rs[slot, k:k + 1, :] = mine[k]

            def s_copy(pd, pt, dy, k, into):
                return pltpu.make_async_remote_copy(
                    src_ref=st.at[dy], dst_ref=rs.at[into], send_sem=ssem, recv_sem=rsem,
                    device_id=(pd, pt), device_id_type=MESH)

            for pd, pt, dy, k in peers:
                s_copy(pd, pt, dy, k, slot).start()
            pltpu.make_async_remote_copy(
                src_ref=pf, dst_ref=pf, send_sem=psend, recv_sem=irecv, device_id=sib, device_id_type=MESH).wait_send()
            id_copy.wait_send()
            with jax.named_scope('wstat'):
                every = rs.at[pl.ds(0, len(peers))]
                stats_copy = pltpu.make_async_remote_copy(
                    src_ref=every, dst_ref=every, send_sem=ssem, recv_sem=rsem, device_id=sib, device_id_type=MESH)
                stats_copy.wait_recv()
            with jax.named_scope('combine'):
                ms = [rs[k, 0:1, :] for k in range(2 * tp)]
                top = ms[0]
                for k in range(1, 2 * tp):
                    top = jnp.maximum(top, ms[k])
                s = jnp.zeros((1, LANES), f32)
                w = s
                p = s
                for k in range(2 * tp):
                    dm = ms[k] - top
                    f = jnp.exp(dm)
                    s = s + f * rs[k, 1:2, :]
                    w = w + f * (rs[k, 2:3, :] + dm * rs[k, 1:2, :])
                    p = p + rs[k, 3:4, :]
                log_sum = jnp.log(s)
                log_norm = top + log_sum
                ent = log_sum - w / s
                logp = p - log_norm
                for k in range(pos):
                    out[k:k + 1, :] = log_norm[:, k * batch:(k + 1) * batch]
                    out[pos + k:pos + k + 1, :] = ent[:, k * batch:(k + 1) * batch]
                    out[2 * pos + k:2 * pos + k + 1, :] = logp[:, k * batch:(k + 1) * batch]
            with jax.named_scope('wsend'):
                stats_copy.wait_send()

        hbm = pl.BlockSpec(memory_space=pl.ANY)
        vmem = pl.BlockSpec(memory_space=pltpu.VMEM)
        dma = pltpu.SemaphoreType.DMA
        bf16 = jnp.bfloat16
        packed = pl.pallas_call(
            kernel,
            out_shape=pltpu.VMEM((3 * pos, batch), f32),
            in_specs=[hbm] * 4,
            out_specs=vmem,
            scratch_shapes=[
                pltpu.VMEM((FIRST, dim), bf16),
                pltpu.VMEM((chunks, CHUNK, dim), bf16),
                pltpu.VMEM((tiles, half, TILE), bf16),
                pltpu.VMEM((rows, dim), bf16),
                pltpu.VMEM((2 * LANES, dim), bf16),
                pltpu.VMEM((parts, rows, LANES), f32),
                pltpu.VMEM((kblocks, rows, LANES), f32),
                pltpu.VMEM((half, 2 * LANES), f32),
                pltpu.VMEM((kblocks, LANES), bf16),
                pltpu.VMEM((kblocks, LANES), f32),
                pltpu.VMEM((drafts, batch), jnp.int32),
                pltpu.VMEM((drafts, batch), jnp.int32),
                pltpu.VMEM((2, 8, LANES), f32),
                pltpu.VMEM((2 * tp, 8, LANES), f32),
                dma((2,)),
                dma((len(STEPS),)),
                dma((4,)),
                dma,
                dma((len(Y_GROUPS),)),
                dma((len(X_GROUPS),)),
                dma((len(STEPS),)),
                dma, dma,
                dma, dma,
            ],
            compiler_params=pltpu.CompilerParams(
                collective_id=0, has_side_effects=True, vmem_limit_bytes=60 * 1024 * 1024),
        )(hidden.transpose(1, 0, 2).reshape(rows, dim), draft_ids.T, norm_gain.reshape(kblocks, LANES), head_w.T)

        def split(src, o_logp, o_logn, o_ent):
            o_logn[...] = src[:pos, :]
            o_ent[...] = src[pos:2 * pos, :]
            o_logp[...] = src[2 * pos:2 * pos + drafts, :]

        logp, logn, ent = pl.pallas_call(
            split,
            out_shape=[jax.ShapeDtypeStruct((drafts, batch), f32), jax.ShapeDtypeStruct((pos, batch), f32),
                       jax.ShapeDtypeStruct((pos, batch), f32)],
            in_specs=[vmem],
            out_specs=[vmem] * 3,
        )(pltpu.with_memory_space_constraint(packed, pltpu.VMEM))
        return logp.T, logn.T, ent.T

    specs_in = (P('dp', None, None), P('dp', None), P(None), P(None, 'tp'))
    specs_out = (P('dp', None), P('dp', None), P('dp', None))
    return jax.shard_map(per_device, mesh=mesh, in_specs=specs_in, out_specs=specs_out, check_vma=False)
```

```python
import jax
import jax.numpy as jnp
from jax import lax
from jax.experimental import pallas as pl
from jax.experimental.pallas import tpu as pltpu
from jax.sharding import PartitionSpec as P

NORM_EPS = 1e-5
MESH = pl.DeviceIdType.MESH
LANES = 128
TILE = 256
BLOCK = 800
OWN = 1600
FIRST = 400
CHUNK = 400
LAST = 320
DIRECT = 6
SHARED = 2
OWN_FORWARDS = ((0,), (1, 2), (3,))
STEPS = (
    ((), (), ('y0', 'a0', 'y1')),
    ((4, 5), (0, 1), ('a1', 'y2', 'x0')),
    ((6, 7), (2, 3), ('a2', 'b0', 'y3', 'x1')),
    ((8, 9), (4, 5), ('a3', 'b1', 'y4', 'x2')),
    ((10, 11), (6, 7), ('a4', 'b2')),
    ((), (), ('y5', 'x3', 'a5', 'b3')),
)
Y_GROUPS = tuple(g for g in OWN_FORWARDS + tuple(ys for ys, _, _ in STEPS) if g)
X_GROUPS = tuple(xs for _, xs, _ in STEPS if xs)


def group_of(groups, i):
    return [i in g for g in groups].index(True)


def step_of(kind, i):
    return [kind + str(i) in names for _, _, names in STEPS].index(True)


NT = (((1,), (1,)), ((), ()))


def update_stats(z, want, carry, first=None):
    z3 = z.reshape(-1, 8, z.shape[-1])
    bm = jnp.max(z3, axis=0)
    m, s, w, p = carry
    for g in range(z3.shape[0]):
        p = jnp.where(want == g, z3[g], p)
    if m is None:
        sh = z3 - bm[None]
        e = jnp.exp(sh)
        return bm, jnp.sum(e, axis=0), jnp.sum(e * sh, axis=0), p
    mn = jnp.maximum(m, bm)
    dm = m - mn
    a = jnp.exp(dm)
    sh = z3 - mn[None]
    e = jnp.exp(sh)
    w = a * (w + dm * s) + jnp.sum(e * sh, axis=0)
    s = a * s + jnp.sum(e, axis=0)
    return mn, s, w, p


def merge_stats(a, b):
    top = jnp.maximum(a[0], b[0])
    da, db = a[0] - top, b[0] - top
    fa, fb = jnp.exp(da), jnp.exp(db)
    return (
        top,
        fa * a[1] + fb * b[1],
        fa * (a[2] + da * a[1]) + fb * (b[2] + db * b[1]),
        a[3] + b[3],
    )


def keep_row(carry, ids):
    m, s, w, p = carry
    sub = lax.broadcasted_iota(jnp.int32, p.shape, 0)
    return m, s, w, jnp.where(sub == jnp.bitwise_and(ids, 7), p, 0.0)


def pack_stats(carry):
    m, s, w, p = carry
    top = jnp.max(m, axis=0, keepdims=True)
    dm = m - top
    f = jnp.exp(dm)
    return (
        top,
        jnp.sum(f * s, axis=0, keepdims=True),
        jnp.sum(f * (w + dm * s), axis=0, keepdims=True),
        jnp.sum(p, axis=0, keepdims=True),
    )


def solution(mesh):
    tp = mesh.shape['tp']

    def per_device(hidden, draft_ids, norm_gain, head_w):
        batch, pos, dim = hidden.shape
        drafts = draft_ids.shape[1]
        cols = head_w.shape[1]
        half = (cols - OWN) // 2
        chunks = (OWN - FIRST) // CHUNK
        rows = batch * pos
        kblocks = dim // LANES
        tiles = dim // TILE
        unique = DIRECT - SHARED
        assert tiles == tp * unique + 2 * SHARED
        parts = 2 * DIRECT
        crossing = 2 * unique
        assert 2 * (parts + crossing) == kblocks
        nblocks = half // BLOCK
        f32 = jnp.float32

        def kernel(x_hbm, ids_hbm, g_hbm, w_hbm, out,
                   hv, ev, wv, xv, nb, nf, pf, acc, gv, gf, idv, idp, st, rs,
                   esem, wsem, lsem, psend, yrecv, xrecv, srecv, isend, irecv, ssem, rsem):
            t = lax.axis_index('tp')
            d = lax.axis_index('dp')
            y = lax.rem(d, 2)
            core = lax.rem(t, 2)
            mate = (d + 1 - 2 * y, t)
            sib = (d, t + 1 - 2 * core)
            nbr_t = lax.rem(t + 2, tp)
            nbr = (d, nbr_t)
            sib_t = t + 1 - 2 * core
            far_t = lax.rem(sib_t + 2, tp)

            cx = pltpu.make_async_copy(x_hbm, xv, lsem.at[0])
            cg = pltpu.make_async_copy(g_hbm, gv, lsem.at[1])
            ci = pltpu.make_async_copy(ids_hbm, idv, lsem.at[2])
            cg.start()
            ci.start()
            for k in range(pos):
                part = pl.ds(k * batch, batch)
                pltpu.make_async_copy(x_hbm.at[part], xv.at[part], lsem.at[0]).start()

            def w_copy(kt, group):
                return pltpu.make_async_copy(
                    w_hbm.at[pl.ds(pl.multiple_of(OWN + y * half, 16), half), pl.ds(pl.multiple_of(kt * TILE, TILE), TILE)],
                    wv.at[kt], wsem.at[group])

            def w_start(group):
                for name in STEPS[group][2]:
                    w_copy(kt_of(name), group).start()

            def w_wait(group):
                some = wv.at[pl.ds(0, len(STEPS[group][2]))]
                pltpu.make_async_copy(some, some, wsem.at[group]).wait()

            def tile_of(owner, i):
                if i < unique:
                    return owner * unique + i
                return tp * unique + lax.rem(owner, 2) * SHARED + i - unique

            def block_of(owner, i):
                return 2 * tile_of(owner, i // 2) + i % 2

            stream_t = {'y': t, 'a': sib_t, 'x': nbr_t, 'b': far_t}

            def kt_of(name):
                return tile_of(stream_t[name[0]], int(name[1:]))

            def e_copy(e):
                return pltpu.make_async_copy(
                    w_hbm.at[pl.ds(pl.multiple_of(FIRST + e * CHUNK, 8), CHUNK), :], ev.at[e], esem.at[lax.rem(e, 2)])

            head_copy = pltpu.make_async_copy(w_hbm.at[pl.ds(0, FIRST), :], hv, lsem.at[3])
            head_copy.start()
            e_copy(0).start()
            barrier = pltpu.get_barrier_semaphore()
            peers = []
            for dy in range(2):
                for k in range(tp):
                    if dy or k:
                        peers.append((mate[0] if dy else d, lax.rem(t + k, tp), dy, k))
            for near in (mate, sib, nbr):
                pl.semaphore_signal(barrier, inc=1, device_id=near, device_id_type=MESH)

            def y_copy(i):
                return pltpu.make_async_remote_copy(
                    src_ref=nf.at[i], dst_ref=pf.at[block_of(t, i)], send_sem=psend, recv_sem=yrecv.at[group_of(Y_GROUPS, i)],
                    device_id=mate, device_id_type=MESH)

            def x_copy(i, owner):
                kb = block_of(owner, i)
                return pltpu.make_async_remote_copy(
                    src_ref=pf.at[kb], dst_ref=pf.at[kb], send_sem=psend, recv_sem=xrecv.at[group_of(X_GROUPS, i)],
                    device_id=nbr, device_id_type=MESH)

            def a_copy(i, owner):
                kb = block_of(owner, i)
                return pltpu.make_async_remote_copy(
                    src_ref=pf.at[kb], dst_ref=pf.at[kb], send_sem=psend, recv_sem=srecv.at[step_of('a', i // 2)],
                    device_id=sib, device_id_type=MESH)

            def b_copy(i, owner):
                kb = block_of(owner, i)
                return pltpu.make_async_remote_copy(
                    src_ref=pf.at[kb], dst_ref=pf.at[kb], send_sem=psend, recv_sem=srecv.at[step_of('b', i // 2)],
                    device_id=sib, device_id_type=MESH)

            def blocks_recv(count, recv):
                some = pf.at[pl.ds(0, count)]
                pltpu.make_async_remote_copy(
                    src_ref=some, dst_ref=some, send_sem=psend, recv_sem=recv,
                    device_id=sib, device_id_type=MESH).wait_recv()

            id_copy = pltpu.make_async_remote_copy(
                src_ref=idv, dst_ref=idp, send_sem=isend, recv_sem=irecv, device_id=mate, device_id_type=MESH)

            nb[rows:LANES, :] = jnp.zeros((LANES - rows, dim), jnp.bfloat16)
            nb[LANES + rows:, :] = jnp.zeros((LANES - rows, dim), jnp.bfloat16)
            with jax.named_scope('waitx'):
                cx.wait()
            sq = jnp.zeros((rows, LANES), f32)
            for k in range(kblocks):
                x = xv[:, k * LANES:(k + 1) * LANES].astype(f32)
                sq = sq + x * x
            inv = lax.rsqrt(jnp.sum(sq, axis=1, keepdims=True) / dim + NORM_EPS)

            with jax.named_scope('waitg'):
                ci.wait()
                cg.wait()
            gf[...] = gv[...].astype(f32)

            def normed(kb):
                x = xv[:, pl.ds(pl.multiple_of(kb * LANES, LANES), LANES)].astype(f32)
                return (x * inv * gf[pl.ds(kb, 1), :]).astype(jnp.bfloat16)

            for i in range(parts):
                nf[i] = normed(block_of(t, i)).astype(f32)
            e_copy(1).start()
            with jax.named_scope('barr'):
                pl.semaphore_wait(barrier, 3)
            for i in range(parts):
                y_copy(i).start()
            id_copy.start()
            for k in range(kblocks):
                nb[:rows, k * LANES:(k + 1) * LANES] = normed(k)

            def forward_y(group):
                if group:
                    blocks_recv(len(group), yrecv.at[group_of(Y_GROUPS, group[0])])
                for i in group:
                    if i < crossing:
                        x_copy(i, t).start()
                    a_copy(i, t).start()

            def forward_x(group):
                if group:
                    blocks_recv(len(group), xrecv.at[group_of(X_GROUPS, group[0])])
                for i in group:
                    b_copy(i, nbr_t).start()

            def sibling_wait(step):
                count = len([name for name in STEPS[step][2] if name[0] in 'ab'])
                if count:
                    blocks_recv(2 * count, srecv.at[step])

            def load_tile(name):
                kt = kt_of(name)
                for h in range(2):
                    nb[LANES:LANES + rows, pl.ds(pl.multiple_of(kt * TILE + h * LANES, LANES), LANES)] = (
                        pf[2 * kt + h].astype(jnp.bfloat16))

            def tiles_dot(names, r):
                z = None
                for name in names:
                    kt = kt_of(name)
                    one = lax.dot_general(wv[kt, r, :], nb[:, pl.ds(pl.multiple_of(kt * TILE, TILE), TILE)], NT,
                                          preferred_element_type=f32)
                    z = one if z is None else z + one
                return z

            pad = jnp.full((1, LANES - drafts * batch), -8, jnp.int32)
            own_ids = jnp.concatenate([idv[k:k + 1, :] - t * cols for k in range(drafts)] + [pad], axis=1)
            own_want = jnp.broadcast_to(jnp.right_shift(own_ids, 3), (8, LANES))
            zero = jnp.zeros((8, LANES), f32)

            def own_forward(e):
                for chunk, blocks in enumerate(OWN_FORWARDS):
                    if blocks:
                        @pl.when(e == chunk)
                        def _():
                            with jax.named_scope('fy'):
                                forward_y(blocks)

            with jax.named_scope('waite'):
                head_copy.wait()
            with jax.named_scope('own'):
                z = lax.dot_general(hv[...], nb[:LANES, :], NT, preferred_element_type=f32)
                own_carry = update_stats(z, own_want, (None, None, None, zero))

            def own_step(e, carry):
                with jax.named_scope('waite'):
                    e_copy(e).wait()

                @pl.when(e + 2 < chunks)
                def _():
                    e_copy(e + 2).start()

                for chunk, groups in ((1, (0,)), (2, (1, 2))):
                    @pl.when(e == chunk)
                    def _():
                        for group in groups:
                            w_start(group)

                with jax.named_scope('own'):
                    pl.delay(1)
                    z = lax.dot_general(ev[e], nb[:LANES, :], NT, preferred_element_type=f32)
                    carry = update_stats(z, own_want - (FIRST + e * CHUNK) // 8, carry)
                own_forward(e)
                return carry

            own_carry = lax.fori_loop(0, chunks, own_step, own_carry)
            own_carry = keep_row(own_carry, own_ids)

            for n_step, (ys, xs, names) in enumerate(STEPS[:-1]):
                with jax.named_scope('fy'):
                    forward_y(ys)
                with jax.named_scope('fx'):
                    forward_x(xs)
                with jax.named_scope('ws'):
                    sibling_wait(n_step)
                for name in names:
                    load_tile(name)
                with jax.named_scope('ww'):
                    w_wait(n_step)
                if n_step + 3 < len(STEPS):
                    w_start(n_step + 3)

                @pl.when(t >= 0)
                def _():
                    with jax.named_scope('step'):
                        for n in range(nblocks):
                            r = slice(n * BLOCK, (n + 1) * BLOCK)
                            z = tiles_dot(names, r)
                            acc[r, :] = z if n_step == 0 else acc[r, :] + z

            id_copy.wait_recv()
            base = t * cols + OWN + y * half
            ids = jnp.concatenate([idv[k:k + 1, :] - base for k in range(drafts)] + [pad]
                                  + [idp[k:k + 1, :] - base for k in range(drafts)] + [pad], axis=1)
            want = jnp.broadcast_to(jnp.right_shift(ids, 3), (8, 2 * LANES))
            sibling_wait(len(STEPS) - 1)
            for name in STEPS[-1][2]:
                load_tile(name)
            with jax.named_scope('ww'):
                w_wait(len(STEPS) - 1)
            carry = (None, None, None, jnp.zeros((8, 2 * LANES), f32))
            with jax.named_scope('final'):
                for n in range(half // LAST):
                    r = slice(n * LAST, (n + 1) * LAST)
                    z = acc[r, :] + tiles_dot(STEPS[-1][2], r)
                    carry = update_stats(z, want - n * LAST // 8, carry)
            carry = keep_row(carry, ids)
            mine = pack_stats(merge_stats(own_carry, [c[:, :LANES] for c in carry]))
            theirs = pack_stats([c[:, LANES:] for c in carry])
            slot = y * tp + t
            for k in range(4):
                st[0, k:k + 1, :] = mine[k]
                st[1, k:k + 1, :] = theirs[k]
                rs[slot, k:k + 1, :] = mine[k]

            def s_copy(pd, pt, dy, k, into):
                return pltpu.make_async_remote_copy(
                    src_ref=st.at[dy], dst_ref=rs.at[into], send_sem=ssem, recv_sem=rsem,
                    device_id=(pd, pt), device_id_type=MESH)

            for pd, pt, dy, k in sorted(peers, key=lambda q: -(2 * q[2] + (q[3] >= 2) + (q[3] == 2))):
                s_copy(pd, pt, dy, k, slot).start()
            pltpu.make_async_remote_copy(
                src_ref=pf, dst_ref=pf, send_sem=psend, recv_sem=irecv, device_id=sib, device_id_type=MESH).wait_send()
            id_copy.wait_send()
            with jax.named_scope('wstat'):
                every = rs.at[pl.ds(0, len(peers))]
                stats_copy = pltpu.make_async_remote_copy(
                    src_ref=every, dst_ref=every, send_sem=ssem, recv_sem=rsem, device_id=sib, device_id_type=MESH)
                stats_copy.wait_recv()
            with jax.named_scope('combine'):
                ms = [rs[k, 0:1, :] for k in range(2 * tp)]
                top = ms[0]
                for k in range(1, 2 * tp):
                    top = jnp.maximum(top, ms[k])
                s = jnp.zeros((1, LANES), f32)
                w = s
                p = s
                for k in range(2 * tp):
                    dm = ms[k] - top
                    f = jnp.exp(dm)
                    s = s + f * rs[k, 1:2, :]
                    w = w + f * (rs[k, 2:3, :] + dm * rs[k, 1:2, :])
                    p = p + rs[k, 3:4, :]
                log_sum = jnp.log(s)
                log_norm = top + log_sum
                ent = log_sum - w / s
                logp = p - log_norm
                for k in range(pos):
                    out[k:k + 1, :] = log_norm[:, k * batch:(k + 1) * batch]
                    out[pos + k:pos + k + 1, :] = ent[:, k * batch:(k + 1) * batch]
                    out[2 * pos + k:2 * pos + k + 1, :] = logp[:, k * batch:(k + 1) * batch]
            with jax.named_scope('wsend'):
                stats_copy.wait_send()

        hbm = pl.BlockSpec(memory_space=pl.ANY)
        vmem = pl.BlockSpec(memory_space=pltpu.VMEM)
        dma = pltpu.SemaphoreType.DMA
        bf16 = jnp.bfloat16
        packed = pl.pallas_call(
            kernel,
            out_shape=pltpu.VMEM((3 * pos, batch), f32),
            in_specs=[hbm] * 4,
            out_specs=vmem,
            scratch_shapes=[
                pltpu.VMEM((FIRST, dim), bf16),
                pltpu.VMEM((chunks, CHUNK, dim), bf16),
                pltpu.VMEM((tiles, half, TILE), bf16),
                pltpu.VMEM((rows, dim), bf16),
                pltpu.VMEM((2 * LANES, dim), bf16),
                pltpu.VMEM((parts, rows, LANES), f32),
                pltpu.VMEM((kblocks, rows, LANES), f32),
                pltpu.VMEM((half, 2 * LANES), f32),
                pltpu.VMEM((kblocks, LANES), bf16),
                pltpu.VMEM((kblocks, LANES), f32),
                pltpu.VMEM((drafts, batch), jnp.int32),
                pltpu.VMEM((drafts, batch), jnp.int32),
                pltpu.VMEM((2, 8, LANES), f32),
                pltpu.VMEM((2 * tp, 8, LANES), f32),
                dma((2,)),
                dma((len(STEPS),)),
                dma((4,)),
                dma,
                dma((len(Y_GROUPS),)),
                dma((len(X_GROUPS),)),
                dma((len(STEPS),)),
                dma, dma,
                dma, dma,
            ],
            compiler_params=pltpu.CompilerParams(
                collective_id=0, has_side_effects=True, vmem_limit_bytes=60 * 1024 * 1024),
        )(hidden.transpose(1, 0, 2).reshape(rows, dim), draft_ids.T, norm_gain.reshape(kblocks, LANES), head_w.T)

        def split(src, o_logp, o_logn, o_ent):
            o_logn[...] = src[:pos, :]
            o_ent[...] = src[pos:2 * pos, :]
            o_logp[...] = src[2 * pos:2 * pos + drafts, :]

        logp, logn, ent = pl.pallas_call(
            split,
            out_shape=[jax.ShapeDtypeStruct((drafts, batch), f32), jax.ShapeDtypeStruct((pos, batch), f32),
                       jax.ShapeDtypeStruct((pos, batch), f32)],
            in_specs=[vmem],
            out_specs=[vmem] * 3,
        )(pltpu.with_memory_space_constraint(packed, pltpu.VMEM))
        return logp.T, logn.T, ent.T

    specs_in = (P('dp', None, None), P('dp', None), P(None), P(None, 'tp'))
    specs_out = (P('dp', None), P('dp', None), P('dp', None))
    return jax.shard_map(per_device, mesh=mesh, in_specs=specs_in, out_specs=specs_out, check_vma=False)
```

```python
import jax
import jax.numpy as jnp
from jax import lax
from jax.experimental import pallas as pl
from jax.experimental.pallas import tpu as pltpu
from jax.sharding import PartitionSpec as P

NORM_EPS = 1e-5
MESH = pl.DeviceIdType.MESH
LANES = 128
TILE = 256
BLOCK = 800
OWN = 1600
FIRST = 400
CHUNK = 400
LAST = 320
DIRECT = 6
SHARED = 2
OWN_FORWARDS = ((0,), (1, 2), (3,))
STEPS = (
    ((), (), ('y0', 'a0', 'y1')),
    ((4, 5), (0, 1), ('a1', 'y2', 'x0')),
    ((6, 7), (2, 3), ('a2', 'b0', 'y3', 'x1')),
    ((8, 9), (4, 5), ('a3', 'b1', 'y4', 'x2')),
    ((10, 11), (6, 7), ('a4', 'b2')),
    ((), (), ('y5', 'x3', 'a5', 'b3')),
)
Y_GROUPS = tuple(g for g in OWN_FORWARDS + tuple(ys for ys, _, _ in STEPS) if g)
X_GROUPS = tuple(xs for _, xs, _ in STEPS if xs)


def group_of(groups, i):
    return [i in g for g in groups].index(True)


def step_of(kind, i):
    return [kind + str(i) in names for _, _, names in STEPS].index(True)


NT = (((1,), (1,)), ((), ()))


def update_stats(z, want, carry, first=None):
    z3 = z.reshape(-1, 8, z.shape[-1])
    bm = jnp.max(z3, axis=0)
    m, s, w, p = carry
    for g in range(z3.shape[0]):
        p = jnp.where(want == g, z3[g], p)
    if m is None:
        sh = z3 - bm[None]
        e = jnp.exp(sh)
        return bm, jnp.sum(e, axis=0), jnp.sum(e * sh, axis=0), p
    mn = jnp.maximum(m, bm)
    dm = m - mn
    a = jnp.exp(dm)
    sh = z3 - mn[None]
    e = jnp.exp(sh)
    w = a * (w + dm * s) + jnp.sum(e * sh, axis=0)
    s = a * s + jnp.sum(e, axis=0)
    return mn, s, w, p


def merge_stats(a, b):
    top = jnp.maximum(a[0], b[0])
    da, db = a[0] - top, b[0] - top
    fa, fb = jnp.exp(da), jnp.exp(db)
    return (
        top,
        fa * a[1] + fb * b[1],
        fa * (a[2] + da * a[1]) + fb * (b[2] + db * b[1]),
        a[3] + b[3],
    )


def keep_row(carry, ids):
    m, s, w, p = carry
    sub = lax.broadcasted_iota(jnp.int32, p.shape, 0)
    return m, s, w, jnp.where(sub == jnp.bitwise_and(ids, 7), p, 0.0)


def pack_stats(carry):
    m, s, w, p = carry
    top = jnp.max(m, axis=0, keepdims=True)
    dm = m - top
    f = jnp.exp(dm)
    return (
        top,
        jnp.sum(f * s, axis=0, keepdims=True),
        jnp.sum(f * (w + dm * s), axis=0, keepdims=True),
        jnp.sum(p, axis=0, keepdims=True),
    )


def solution(mesh):
    tp = mesh.shape['tp']

    def per_device(hidden, draft_ids, norm_gain, head_w):
        batch, pos, dim = hidden.shape
        drafts = draft_ids.shape[1]
        cols = head_w.shape[1]
        half = (cols - OWN) // 2
        chunks = (OWN - FIRST) // CHUNK
        rows = batch * pos
        kblocks = dim // LANES
        tiles = dim // TILE
        unique = DIRECT - SHARED
        assert tiles == tp * unique + 2 * SHARED
        parts = 2 * DIRECT
        crossing = 2 * unique
        assert 2 * (parts + crossing) == kblocks
        nblocks = half // BLOCK
        f32 = jnp.float32

        def kernel(x_hbm, ids_hbm, g_hbm, w_hbm, out,
                   hv, ev, wv, xv, nb, nf, pf, acc, gv, gf, idv, idp, st, rs,
                   esem, wsem, lsem, psend, yrecv, xrecv, srecv, isend, irecv, ssem, rsem):
            t = lax.axis_index('tp')
            d = lax.axis_index('dp')
            y = lax.rem(d, 2)
            core = lax.rem(t, 2)
            mate = (d + 1 - 2 * y, t)
            sib = (d, t + 1 - 2 * core)
            nbr_t = lax.rem(t + 2, tp)
            nbr = (d, nbr_t)
            sib_t = t + 1 - 2 * core
            far_t = lax.rem(sib_t + 2, tp)

            cx = pltpu.make_async_copy(x_hbm, xv, lsem.at[0])
            cg = pltpu.make_async_copy(g_hbm, gv, lsem.at[1])
            ci = pltpu.make_async_copy(ids_hbm, idv, lsem.at[2])
            for k in range(pos):
                part = pl.ds(k * batch, batch)
                pltpu.make_async_copy(x_hbm.at[part], xv.at[part], lsem.at[0]).start()
            cg.start()
            ci.start()

            def w_copy(kt, group):
                return pltpu.make_async_copy(
                    w_hbm.at[pl.ds(pl.multiple_of(OWN + y * half, 16), half), pl.ds(pl.multiple_of(kt * TILE, TILE), TILE)],
                    wv.at[kt], wsem.at[group % 3])

            def w_start(group):
                for name in STEPS[group][2]:
                    w_copy(kt_of(name), group).start()

            def w_wait(group):
                some = wv.at[pl.ds(0, len(STEPS[group][2]))]
                pltpu.make_async_copy(some, some, wsem.at[group % 3]).wait()

            def tile_of(owner, i):
                if i < unique:
                    return owner * unique + i
                return tp * unique + lax.rem(owner, 2) * SHARED + i - unique

            def block_of(owner, i):
                return 2 * tile_of(owner, i // 2) + i % 2

            stream_t = {'y': t, 'a': sib_t, 'x': nbr_t, 'b': far_t}

            def kt_of(name):
                return tile_of(stream_t[name[0]], int(name[1:]))

            def e_copy(e):
                return pltpu.make_async_copy(
                    w_hbm.at[pl.ds(pl.multiple_of(FIRST + e * CHUNK, 8), CHUNK), :], ev.at[e], esem.at[lax.rem(e, 2)])

            head_copy = pltpu.make_async_copy(w_hbm.at[pl.ds(0, FIRST), :], hv, lsem.at[3])
            head_copy.start()
            e_copy(0).start()
            barrier = pltpu.get_barrier_semaphore()
            peers = []
            for dy in range(2):
                for k in range(tp):
                    if dy or k:
                        peers.append((mate[0] if dy else d, lax.rem(t + k, tp), dy, k))
            for near in (mate, sib, nbr):
                pl.semaphore_signal(barrier, inc=1, device_id=near, device_id_type=MESH)

            def y_copy(i):
                return pltpu.make_async_remote_copy(
                    src_ref=nf.at[i], dst_ref=pf.at[block_of(t, i)], send_sem=psend, recv_sem=yrecv.at[group_of(Y_GROUPS, i)],
                    device_id=mate, device_id_type=MESH)

            def x_copy(i, owner):
                kb = block_of(owner, i)
                return pltpu.make_async_remote_copy(
                    src_ref=pf.at[kb], dst_ref=pf.at[kb], send_sem=psend, recv_sem=xrecv.at[group_of(X_GROUPS, i)],
                    device_id=nbr, device_id_type=MESH)

            def a_copy(i, owner):
                kb = block_of(owner, i)
                return pltpu.make_async_remote_copy(
                    src_ref=pf.at[kb], dst_ref=pf.at[kb], send_sem=psend, recv_sem=srecv.at[step_of('a', i // 2)],
                    device_id=sib, device_id_type=MESH)

            def b_copy(i, owner):
                kb = block_of(owner, i)
                return pltpu.make_async_remote_copy(
                    src_ref=pf.at[kb], dst_ref=pf.at[kb], send_sem=psend, recv_sem=srecv.at[step_of('b', i // 2)],
                    device_id=sib, device_id_type=MESH)

            def blocks_recv(count, recv):
                some = pf.at[pl.ds(0, count)]
                pltpu.make_async_remote_copy(
                    src_ref=some, dst_ref=some, send_sem=psend, recv_sem=recv,
                    device_id=sib, device_id_type=MESH).wait_recv()

            id_copy = pltpu.make_async_remote_copy(
                src_ref=idv, dst_ref=idp, send_sem=isend, recv_sem=irecv, device_id=mate, device_id_type=MESH)

            nb[rows:LANES, :] = jnp.zeros((LANES - rows, dim), jnp.bfloat16)
            nb[LANES + rows:, :] = jnp.zeros((LANES - rows, dim), jnp.bfloat16)
            with jax.named_scope('waitx'):
                cx.wait()
            sq = jnp.zeros((rows, LANES), f32)
            for k in range(kblocks):
                x = xv[:, k * LANES:(k + 1) * LANES].astype(f32)
                sq = sq + x * x
            inv = lax.rsqrt(jnp.sum(sq, axis=1, keepdims=True) / dim + NORM_EPS)

            with jax.named_scope('waitg'):
                ci.wait()
                cg.wait()
            gf[...] = gv[...].astype(f32)

            def normed(kb):
                x = xv[:, pl.ds(pl.multiple_of(kb * LANES, LANES), LANES)].astype(f32)
                return (x * inv * gf[pl.ds(kb, 1), :]).astype(jnp.bfloat16)

            for i in range(parts):
                nf[i] = normed(block_of(t, i)).astype(f32)
            e_copy(1).start()
            with jax.named_scope('barr'):
                pl.semaphore_wait(barrier, 3)
            for i in range(parts):
                y_copy(i).start()
            id_copy.start()
            for k in range(kblocks):
                nb[:rows, k * LANES:(k + 1) * LANES] = normed(k)

            def forward_y(group):
                if group:
                    blocks_recv(len(group), yrecv.at[group_of(Y_GROUPS, group[0])])
                for i in group:
                    if i < crossing:
                        x_copy(i, t).start()
                    a_copy(i, t).start()

            def forward_x(group):
                if group:
                    blocks_recv(len(group), xrecv.at[group_of(X_GROUPS, group[0])])
                for i in group:
                    b_copy(i, nbr_t).start()

            def sibling_wait(step):
                count = len([name for name in STEPS[step][2] if name[0] in 'ab'])
                if count:
                    blocks_recv(2 * count, srecv.at[step])

            def load_tile(name):
                kt = kt_of(name)
                for h in range(2):
                    nb[LANES:LANES + rows, pl.ds(pl.multiple_of(kt * TILE + h * LANES, LANES), LANES)] = (
                        pf[2 * kt + h].astype(jnp.bfloat16))

            def tiles_dot(names, r):
                z = None
                for name in names:
                    kt = kt_of(name)
                    one = lax.dot_general(wv[kt, r, :], nb[:, pl.ds(pl.multiple_of(kt * TILE, TILE), TILE)], NT,
                                          preferred_element_type=f32)
                    z = one if z is None else z + one
                return z

            pad = jnp.full((1, LANES - drafts * batch), -8, jnp.int32)
            own_ids = jnp.concatenate([idv[k:k + 1, :] - t * cols for k in range(drafts)] + [pad], axis=1)
            own_want = jnp.broadcast_to(jnp.right_shift(own_ids, 3), (8, LANES))
            zero = jnp.zeros((8, LANES), f32)

            def own_forward(e):
                for chunk, blocks in enumerate(OWN_FORWARDS):
                    if blocks:
                        @pl.when(e == chunk)
                        def _():
                            with jax.named_scope('fy'):
                                forward_y(blocks)

            with jax.named_scope('waite'):
                head_copy.wait()
            with jax.named_scope('own'):
                z = lax.dot_general(hv[...], nb[:LANES, :], NT, preferred_element_type=f32)
                own_carry = update_stats(z, own_want, (None, None, None, zero))

            def own_step(e, carry):
                with jax.named_scope('waite'):
                    e_copy(e).wait()

                @pl.when(e + 2 < chunks)
                def _():
                    e_copy(e + 2).start()

                for chunk, groups in ((1, (0,)), (2, (1, 2))):
                    @pl.when(e == chunk)
                    def _():
                        for group in groups:
                            w_start(group)

                with jax.named_scope('own'):
                    pl.delay(1)
                    z = lax.dot_general(ev[e], nb[:LANES, :], NT, preferred_element_type=f32)
                    carry = update_stats(z, own_want - (FIRST + e * CHUNK) // 8, carry)
                own_forward(e)
                return carry

            own_carry = lax.fori_loop(0, chunks, own_step, own_carry)
            own_carry = keep_row(own_carry, own_ids)

            for n_step, (ys, xs, names) in enumerate(STEPS[:-1]):
                with jax.named_scope('fy'):
                    forward_y(ys)
                with jax.named_scope('fx'):
                    forward_x(xs)
                with jax.named_scope('ws'):
                    sibling_wait(n_step)
                for name in names:
                    load_tile(name)
                with jax.named_scope('ww'):
                    w_wait(n_step)
                if n_step + 3 < len(STEPS):
                    w_start(n_step + 3)

                @pl.when(t >= 0)
                def _():
                    with jax.named_scope('step'):
                        for n in range(nblocks):
                            r = slice(n * BLOCK, (n + 1) * BLOCK)
                            z = tiles_dot(names, r)
                            acc[r, :] = z if n_step == 0 else acc[r, :] + z

            id_copy.wait_recv()
            base = t * cols + OWN + y * half
            ids = jnp.concatenate([idv[k:k + 1, :] - base for k in range(drafts)] + [pad]
                                  + [idp[k:k + 1, :] - base for k in range(drafts)] + [pad], axis=1)
            want = jnp.broadcast_to(jnp.right_shift(ids, 3), (8, 2 * LANES))
            sibling_wait(len(STEPS) - 1)
            for name in STEPS[-1][2]:
                load_tile(name)
            with jax.named_scope('ww'):
                w_wait(len(STEPS) - 1)
            carry = (None, None, None, jnp.zeros((8, 2 * LANES), f32))
            with jax.named_scope('final'):
                for n in range(half // LAST):
                    r = slice(n * LAST, (n + 1) * LAST)
                    z = acc[r, :] + tiles_dot(STEPS[-1][2], r)
                    carry = update_stats(z, want - n * LAST // 8, carry)
            carry = keep_row(carry, ids)
            mine = pack_stats(merge_stats(own_carry, [c[:, :LANES] for c in carry]))
            theirs = pack_stats([c[:, LANES:] for c in carry])
            slot = y * tp + t
            for k in range(4):
                st[0, k:k + 1, :] = mine[k]
                st[1, k:k + 1, :] = theirs[k]
                rs[slot, k:k + 1, :] = mine[k]

            def s_copy(pd, pt, dy, k, into):
                return pltpu.make_async_remote_copy(
                    src_ref=st.at[dy], dst_ref=rs.at[into], send_sem=ssem, recv_sem=rsem,
                    device_id=(pd, pt), device_id_type=MESH)

            for pd, pt, dy, k in sorted(peers, key=lambda q: -(2 * q[2] + (q[3] >= 2) + (q[3] == 2))):
                s_copy(pd, pt, dy, k, slot).start()
            pltpu.make_async_remote_copy(
                src_ref=pf, dst_ref=pf, send_sem=psend, recv_sem=irecv, device_id=sib, device_id_type=MESH).wait_send()
            id_copy.wait_send()
            with jax.named_scope('wstat'):
                every = rs.at[pl.ds(0, len(peers))]
                stats_copy = pltpu.make_async_remote_copy(
                    src_ref=every, dst_ref=every, send_sem=ssem, recv_sem=rsem, device_id=sib, device_id_type=MESH)
                stats_copy.wait_recv()
            with jax.named_scope('combine'):
                ms = [rs[k, 0:1, :] for k in range(2 * tp)]
                top = ms[0]
                for k in range(1, 2 * tp):
                    top = jnp.maximum(top, ms[k])
                s = jnp.zeros((1, LANES), f32)
                w = s
                p = s
                for k in range(2 * tp):
                    dm = ms[k] - top
                    f = jnp.exp(dm)
                    s = s + f * rs[k, 1:2, :]
                    w = w + f * (rs[k, 2:3, :] + dm * rs[k, 1:2, :])
                    p = p + rs[k, 3:4, :]
                log_sum = jnp.log(s)
                log_norm = top + log_sum
                ent = log_sum - w / s
                logp = p - log_norm
                for k in range(pos):
                    out[k:k + 1, :] = log_norm[:, k * batch:(k + 1) * batch]
                    out[pos + k:pos + k + 1, :] = ent[:, k * batch:(k + 1) * batch]
                    out[2 * pos + k:2 * pos + k + 1, :] = logp[:, k * batch:(k + 1) * batch]
            with jax.named_scope('wsend'):
                stats_copy.wait_send()

        hbm = pl.BlockSpec(memory_space=pl.ANY)
        vmem = pl.BlockSpec(memory_space=pltpu.VMEM)
        dma = pltpu.SemaphoreType.DMA
        bf16 = jnp.bfloat16
        packed = pl.pallas_call(
            kernel,
            out_shape=pltpu.VMEM((3 * pos, batch), f32),
            in_specs=[hbm] * 4,
            out_specs=vmem,
            scratch_shapes=[
                pltpu.VMEM((FIRST, dim), bf16),
                pltpu.VMEM((chunks, CHUNK, dim), bf16),
                pltpu.VMEM((tiles, half, TILE), bf16),
                pltpu.VMEM((rows, dim), bf16),
                pltpu.VMEM((2 * LANES, dim), bf16),
                pltpu.VMEM((parts, rows, LANES), f32),
                pltpu.VMEM((kblocks, rows, LANES), f32),
                pltpu.VMEM((half, 2 * LANES), f32),
                pltpu.VMEM((kblocks, LANES), bf16),
                pltpu.VMEM((kblocks, LANES), f32),
                pltpu.VMEM((drafts, batch), jnp.int32),
                pltpu.VMEM((drafts, batch), jnp.int32),
                pltpu.VMEM((2, 8, LANES), f32),
                pltpu.VMEM((2 * tp, 8, LANES), f32),
                dma((2,)),
                dma((3,)),
                dma((4,)),
                dma,
                dma((len(Y_GROUPS),)),
                dma((len(X_GROUPS),)),
                dma((len(STEPS),)),
                dma, dma,
                dma, dma,
            ],
            compiler_params=pltpu.CompilerParams(
                collective_id=0, has_side_effects=True, vmem_limit_bytes=60 * 1024 * 1024),
        )(hidden.transpose(1, 0, 2).reshape(rows, dim), draft_ids.T, norm_gain.reshape(kblocks, LANES), head_w.T)

        def split(src, o_logp, o_logn, o_ent):
            o_logn[...] = src[:pos, :]
            o_ent[...] = src[pos:2 * pos, :]
            o_logp[...] = src[2 * pos:2 * pos + drafts, :]

        logp, logn, ent = pl.pallas_call(
            split,
            out_shape=[jax.ShapeDtypeStruct((drafts, batch), f32), jax.ShapeDtypeStruct((pos, batch), f32),
                       jax.ShapeDtypeStruct((pos, batch), f32)],
            in_specs=[vmem],
            out_specs=[vmem] * 3,
        )(pltpu.with_memory_space_constraint(packed, pltpu.VMEM))
        return logp.T, logn.T, ent.T

    specs_in = (P('dp', None, None), P('dp', None), P(None), P(None, 'tp'))
    specs_out = (P('dp', None), P('dp', None), P('dp', None))
    return jax.shard_map(per_device, mesh=mesh, in_specs=specs_in, out_specs=specs_out, check_vma=False)
```
